128 devices in a mesh: row: 32 (over y, z, core), col: 4 (over x).
Axes of the slice: x: 4, y: 4, z: 4, core: 2. Of those that a mesh axis runs over, the one named last changes fastest.
Arguments:
- acts_in: bfloat16 [32768, 4608], P('row'), may hold values from -64 to 64
- grad_query: bfloat16 [32768, 4096], P('row', 'col'), may hold values from -1.41421356 to 1.41421356
- attn_out: bfloat16 [32768, 4096], P('row'), may hold values from -64 to 64
- grad_out: bfloat16 [32768, 4608], P('row', 'col'), may hold values from -1.41421356 to 1.41421356
- row_query: float32 [4608], P('row'), may hold values from 0.05 to 18
- col_query: float32 [4096], P('col'), may hold values from 0.05 to 2
- row_output: float32 [4096], P('row'), may hold values from 0.05 to 18
- col_output: float32 [4608], P('col'), may hold values from 0.05 to 2
Outputs:
- update_query: bfloat16 [4608, 4096], P('row', 'col')
- update_output: bfloat16 [4096, 4608], P('row', 'col')
- new_row_query: float32 [4608], P('row')
- new_col_query: float32 [4096], P('col')
- new_row_output: float32 [4096], P('row')
- new_col_output: float32 [4608], P('col')
The draws below stay inside these ranges and needn't reach their ends.
All inputs are finite; a program needn't handle non-finite values.
Results may differ from the reference program's by a relative error of at most 0.028.
Values may be sent and summed in bfloat16 or wider, within the bound.
No kernel may reach another device: no remote copies, remote signals or barrier semaphores. Data moves between devices by JAX's collectives and lax.ppermute only.
A program may use at most 128 MiB of HBM per device.

```python
import math
import jax
import jax.numpy as jnp
from jax import lax

D = 4608
Q = 4096
TOK_DEV = 1024
CLIP = 3072
TOKENS = 32768
N_ROW = 32


def scaled_field(key, row_count, col_count, size_scale):
    key_list = jax.random.split(key, 2)
    col_scale = jnp.exp(jax.random.uniform(key_list[1], (col_count,), jnp.float32, 0.0, math.log(10.0)))
    col_scale = col_scale * jnp.exp(math.log(3.0) * jnp.arange(col_count, dtype=jnp.float32) / col_count)
    col_scale = col_scale / jnp.sqrt(jnp.mean(col_scale * col_scale))
    base_field = jax.random.normal(key_list[0], (row_count, col_count), jnp.float32)
    field_bound = 64.0 * size_scale
    return jnp.clip(base_field * col_scale * size_scale, -field_bound, field_bound).astype(jnp.bfloat16)


def rising_factor(key, count):
    base_value = jnp.exp(jax.random.uniform(key, (count,), jnp.float32, math.log(0.05), math.log(2.0)))
    ramp = jnp.exp(math.log(9.0) * jnp.arange(count, dtype=jnp.float32) / count)
    return jnp.clip(base_value * ramp, 0.05, 18.0)


def draw_acts_in(key, part):
    return scaled_field(jax.random.fold_in(key, 11), TOKENS, D, 1.0)


def draw_grad_query(key, part):
    return scaled_field(jax.random.fold_in(key, 12), TOKENS, Q, 4.0 / math.sqrt(TOKENS))


def draw_attn_out(key, part):
    return scaled_field(jax.random.fold_in(key, 13), TOKENS, Q, 1.0)


def draw_grad_out(key, part):
    return scaled_field(jax.random.fold_in(key, 14), TOKENS, D, 4.0 / math.sqrt(TOKENS))


def draw_row_query(key, part):
    return rising_factor(jax.random.fold_in(key, 15), D)


def draw_row_output(key, part):
    return rising_factor(jax.random.fold_in(key, 16), Q)


def levels(rng, shape, shards, low, top_value):
    loudness = 1.0
    for dim, blocks in shards:
        heights = jax.random.uniform(jax.random.fold_in(jax.random.fold_in(rng, 6), dim), (blocks,), jnp.float32, low / len(shards), top_value / len(shards))
        loudness = loudness * jnp.repeat(jnp.exp(heights), shape[dim] // blocks).reshape((-1,) + (1,) * (len(shape) - 1 - dim))
    return loudness


def setup_inputs(seed: int = 0) -> dict:
    seeds = jax.random.split(jax.random.key(seed), 9)
    acts_in = draw_acts_in(jax.random.fold_in(seeds[8], 71), 0)
    grad_query = draw_grad_query(jax.random.fold_in(seeds[8], 71), 0)
    attn_out = draw_attn_out(jax.random.fold_in(seeds[8], 71), 0)
    grad_out = draw_grad_out(jax.random.fold_in(seeds[8], 71), 0)
    row_query = draw_row_query(jax.random.fold_in(seeds[8], 71), 0)
    col_query = jnp.clip(jnp.exp(math.log(2.0) - 3.6888794 * jax.random.uniform(seeds[5], (Q,), jnp.float32) ** levels(seeds[5], (Q,), ((0, 4),), -0.2, 0.2)), 0.05, 2.0)
    row_output = draw_row_output(jax.random.fold_in(seeds[8], 71), 0)
    col_output = jnp.clip(jnp.exp(math.log(2.0) - 3.6888794 * jax.random.uniform(seeds[7], (D,), jnp.float32) ** levels(seeds[7], (D,), ((0, 4),), -0.2, 0.2)), 0.05, 2.0)
    return dict(acts_in=acts_in, grad_query=grad_query, attn_out=attn_out, grad_out=grad_out, row_query=row_query, col_query=col_query, row_output=row_output, col_output=col_output)


decay_rate = 0.81
epsilon_one = 1e-30

def grouped_gradient(left, right):
    left_groups = left.astype(jnp.float32).reshape(N_ROW, TOK_DEV, left.shape[1])
    right_groups = right.astype(jnp.float32).reshape(N_ROW, TOK_DEV, right.shape[1])

    def add_group(running, paired):
        partial_grad = jnp.dot(paired[0].T, paired[1], precision=lax.Precision.HIGHEST, preferred_element_type=jnp.float32)
        rounded = lax.optimization_barrier(partial_grad.astype(jnp.bfloat16))
        return (running + rounded.astype(jnp.float32), None)
    initial = jnp.zeros((left.shape[1], right.shape[1]), jnp.float32)
    summed, unused = lax.scan(add_group, initial, (left_groups, right_groups))
    return summed

def factored_update(gradient, clip_scale, row_old, col_old):
    clipped = clip_scale * gradient
    squared = clipped * clipped + epsilon_one
    row_new = decay_rate * row_old + (1.0 - decay_rate) * lax.optimization_barrier(jnp.mean(squared, axis=1))
    col_new = decay_rate * col_old + (1.0 - decay_rate) * lax.optimization_barrier(jnp.mean(squared, axis=0))
    row_level = jnp.mean(row_new)
    update = clipped * lax.rsqrt(row_new[:, None] * col_new[None, :] / row_level)
    return (update.astype(jnp.bfloat16), row_new, col_new)

def reference(acts_in, grad_query, attn_out, grad_out, row_query, col_query, row_output, col_output):
    query_grad = grouped_gradient(acts_in, grad_query)
    output_grad = grouped_gradient(attn_out, grad_out)
    grad_norm = jnp.sqrt(jnp.sum(query_grad * query_grad) + jnp.sum(output_grad * output_grad))
    clip_scale = CLIP / jnp.maximum(grad_norm, jnp.float32(CLIP))
    update_query, new_row_query, new_col_query = factored_update(query_grad, clip_scale, row_query, col_query)
    update_output, new_row_output, new_col_output = factored_update(output_grad, clip_scale, row_output, col_output)
    return (update_query, update_output, new_row_query, new_col_query, new_row_output, new_col_output)
```

```python
import functools

import jax
import jax.numpy as jnp
from jax import lax
from jax.experimental import pallas as pl
from jax.experimental.pallas import tpu as pltpu
from jax.sharding import Mesh
from jax.sharding import PartitionSpec as P

CLIP = 3072
ROW = ("row_0", "row_1", "row_2")

decay_rate = 0.81
epsilon_one = 1e-30


def shift(value, axis, by):
    size = lax.axis_size(axis)
    return lax.ppermute(value, axis, [(i, (i + by) % size) for i in range(size)])


def slab_kernel(slabs, pieces, group, where_ref, left_ref, right_ref, *rest):
    blocks = len(slabs)
    outs, (left_buf, out_buf, in_sem, out_sem) = rest[: 2 * blocks], rest[2 * blocks :]
    core = where_ref[0]
    arrivals = []
    for b, block in enumerate(slabs):
        offset = 0
        for s, runs in enumerate(block):
            waits = []
            at = 0
            for r, (index, plus, width) in enumerate(runs):
                start = pl.multiple_of(where_ref[index] + plus, 128)
                copy = pltpu.make_async_copy(
                    left_ref.at[:, pl.ds(start, width)],
                    left_buf.at[b * pieces + s, :, pl.ds(at, width)],
                    in_sem.at[b * pieces + s, r],
                )
                copy.start()
                waits.append(copy)
                at += width
            arrivals.append((b, s, offset, at, waits))
            offset += at
    leaving = []
    sent = 0
    for b, s, offset, width, waits in arrivals:
        if s == 0:
            sent = 0
        for copy in waits:
            copy.wait()
        product = lax.dot_general(
            left_buf[b * pieces + s],
            right_ref[...],
            (((0,), (0,)), ((), ())),
            preferred_element_type=jnp.float32,
        )
        out_buf[b, pl.ds(offset, width), :] = product.astype(jnp.bfloat16)
        while (sent + 1) * group <= offset + width:
            source = out_buf.at[b, pl.ds(sent * group, group), :]
            keep = outs[2 * b].at[sent // 2]
            give = outs[2 * b + 1].at[sent // 2]
            sem = out_sem.at[b, sent]
            mine = core == sent % 2

            @pl.when(mine)
            def _(source=source, keep=keep, sem=sem):
                pltpu.make_async_copy(source, keep, sem).start()

            @pl.when(jnp.logical_not(mine))
            def _(source=source, give=give, sem=sem):
                pltpu.make_async_copy(source, give, sem).start()

            leaving.append((source, keep, sem))
            sent += 1
    for source, keep, sem in leaving:
        pltpu.make_async_copy(source, keep, sem).wait()


def partial_blocks(where, left, right, slabs, group, name):
    tokens, columns = right.shape
    blocks, pieces = len(slabs), len(slabs[0])
    width = sum(w for _, _, w in slabs[0][0])
    runs = max(len(r) for r in slabs[0])
    rows = width * pieces
    shape = jax.ShapeDtypeStruct((rows // group // 2, group, columns), jnp.bfloat16)
    vmem = 2 * (blocks * rows * (tokens + columns) + 2 * tokens * columns) + 6 * 1024 * 1024 + 8 * width * columns
    outs = pl.pallas_call(
        functools.partial(slab_kernel, slabs, pieces, group),
        out_shape=[shape] * (2 * blocks),
        in_specs=[
            pl.BlockSpec(memory_space=pltpu.SMEM),
            pl.BlockSpec(memory_space=pl.ANY),
            pl.BlockSpec(memory_space=pltpu.VMEM),
        ],
        out_specs=[pl.BlockSpec(memory_space=pl.ANY)] * (2 * blocks),
        scratch_shapes=[
            pltpu.VMEM((blocks * pieces, tokens, width), jnp.bfloat16),
            pltpu.VMEM((blocks, rows, columns), jnp.bfloat16),
            pltpu.SemaphoreType.DMA((blocks * pieces, runs)),
            pltpu.SemaphoreType.DMA((blocks, rows // group)),
        ],
        compiler_params=pltpu.CompilerParams(vmem_limit_bytes=vmem),
        cost_estimate=pl.CostEstimate(
            flops=2 * blocks * rows * tokens * columns,
            bytes_accessed=2 * (blocks * rows * (tokens + columns) + tokens * columns),
            transcendentals=0,
        ),
        name=name,
    )(where, left, right)
    return [(outs[2 * b], outs[2 * b + 1]) for b in range(blocks)]


def wide(value):
    return value.astype(jnp.float32)


def narrow(value):
    return value.astype(jnp.bfloat16)


def sum_to_owner(parts, first, second, position):
    half = parts[0][0].shape[-1] // 2
    low, high = slice(0, half), slice(half, 2 * half)

    def own(k, columns):
        kept, other = parts[k]
        return wide(kept[..., columns]) + wide(other[..., columns])

    far_low = shift(narrow(own(2, low)), first, 1)
    far_high = shift(narrow(own(2, high)), first, -1)
    near_high = shift(narrow(own(1, high)), first, 1)
    near_low = shift(narrow(own(3, low)), first, -1)
    next_low = shift(narrow(own(1, low) + wide(far_low)), first, 1)
    next_high = shift(narrow(own(3, high) + wide(far_high)), first, -1)
    total = jnp.concatenate(
        [
            own(0, low) + wide(next_low) + wide(near_low),
            own(0, high) + wide(next_high) + wide(near_high),
        ],
        axis=-1,
    )

    def toward(k):
        return lax.dynamic_index_in_dim(total, lax.rem(position + k, 4), 0, keepdims=False)

    arrived = [shift(narrow(toward(k)), second, k) for k in (2, 1, 3)]
    return toward(0) + wide(arrived[0]) + wide(arrived[1]) + wide(arrived[2])


def all_sum(value, axis):
    size = lax.axis_size(axis)
    total = value
    for k in range(1, size):
        total = total + shift(value, axis, k)
    return total


def finish(
    gradient, clip_scale, row_old, col_old, row_sums, col_sums, row_level, whole_rows, whole_cols
):
    squared_scale = clip_scale * clip_scale
    row_new = decay_rate * row_old + (1.0 - decay_rate) * (
        squared_scale * row_sums / whole_cols + epsilon_one
    )
    col_new = decay_rate * col_old + (1.0 - decay_rate) * (
        squared_scale * col_sums / whole_rows + epsilon_one
    )
    update = clip_scale * gradient * lax.rsqrt(row_new[:, None] * col_new[None, :] / row_level)
    return (update.astype(jnp.bfloat16), row_new, col_new)


def shards(acts_in, grad_query, attn_out, grad_out, row_query, col_query, row_output, col_output):
    query_rows = row_query.shape[0]
    output_rows = row_output.shape[0]
    query_width = col_query.shape[0]
    output_width = col_output.shape[0]
    y, z, core = lax.axis_index("row_0"), lax.axis_index("row_1"), lax.axis_index("row_2")
    pair_query, pair_output = 2 * query_rows, 2 * output_rows
    where = jnp.stack(
        [core]
        + [lax.rem(y + k, 4) * (4 * pair_query) for k in range(4)]
        + [lax.rem(z + k, 4) * pair_output for k in range(4)]
    ).astype(jnp.int32)

    piece = 4 * pair_query // 3

    def query_slabs(k):
        return [[(1 + k, s * piece, piece)] for s in range(3)]

    def output_slabs(k):
        run = lambda i: (5 + k, i * 4 * pair_output, pair_output)
        return [[run(0), run(1)], [run(2), run(3)]]

    query_parts, output_parts = {}, {}
    for ks in ((2,), (1, 3), (0,)):
        tag = "_".join(map(str, ks))
        for parts, left, right, slabs, group, name in (
            (query_parts, acts_in, grad_query, query_slabs, query_rows, "query"),
            (output_parts, attn_out, grad_out, output_slabs, output_rows, "output"),
        ):
            made = partial_blocks(where, left, right, [slabs(k) for k in ks], group, f"{name}_{tag}")
            for k, (keep, give) in zip(ks, made):
                parts[k] = (keep, shift(give, "row_2", 1))

    query_grad = sum_to_owner(query_parts, "row_0", "row_1", z)
    output_grad = sum_to_owner(output_parts, "row_1", "row_0", y)

    query_whole_rows = query_rows * lax.axis_size(ROW)
    output_whole_rows = output_rows * lax.axis_size(ROW)
    query_whole_cols = query_width * lax.axis_size("col")
    output_whole_cols = output_width * lax.axis_size("col")
    query_square = query_grad * query_grad
    output_square = output_grad * output_grad
    query_rowsum = jnp.sum(query_square, axis=1)
    output_rowsum = jnp.sum(output_square, axis=1)
    query_colsum = jnp.sum(query_square, axis=0)
    output_colsum = jnp.sum(output_square, axis=0)
    rowsums = all_sum(jnp.concatenate([query_rowsum, output_rowsum]), "col")
    query_rowsum, output_rowsum = rowsums[:query_rows], rowsums[query_rows:]
    scalars = jnp.stack(
        [jnp.sum(query_rowsum), jnp.sum(output_rowsum), jnp.sum(row_query), jnp.sum(row_output)]
    )
    sums = jnp.concatenate([query_colsum, output_colsum, scalars])
    for axis in ("row_2", "row_0", "row_1"):
        sums = all_sum(sums, axis)
    query_colsum = sums[:query_width]
    output_colsum = sums[query_width : query_width + output_width]
    query_squares, output_squares, query_oldsum, output_oldsum = (
        sums[query_width + output_width + i] for i in range(4)
    )
    clip_scale = CLIP / jnp.maximum(jnp.sqrt(query_squares + output_squares), jnp.float32(CLIP))
    squared_scale = clip_scale * clip_scale
    query_level = decay_rate * query_oldsum / query_whole_rows + (1.0 - decay_rate) * (
        squared_scale * query_squares / (query_whole_rows * query_whole_cols) + epsilon_one
    )
    output_level = decay_rate * output_oldsum / output_whole_rows + (1.0 - decay_rate) * (
        squared_scale * output_squares / (output_whole_rows * output_whole_cols) + epsilon_one
    )
    update_query, new_row_query, new_col_query = finish(
        query_grad,
        clip_scale,
        row_query,
        col_query,
        query_rowsum,
        query_colsum,
        query_level,
        query_whole_rows,
        query_whole_cols,
    )
    update_output, new_row_output, new_col_output = finish(
        output_grad,
        clip_scale,
        row_output,
        col_output,
        output_rowsum,
        output_colsum,
        output_level,
        output_whole_rows,
        output_whole_cols,
    )
    return (
        update_query,
        update_output,
        new_row_query,
        new_col_query,
        new_row_output,
        new_col_output,
    )


def solution(mesh):
    split = Mesh(
        mesh.devices.reshape(4, 4, 2, mesh.shape["col"]), ("row_0", "row_1", "row_2", "col")
    )
    return jax.shard_map(
        shards,
        mesh=split,
        in_specs=(
            P(ROW, None),
            P(ROW, "col"),
            P(ROW, None),
            P(ROW, "col"),
            P(ROW),
            P("col"),
            P(ROW),
            P("col"),
        ),
        out_specs=(P(ROW, "col"), P(ROW, "col"), P(ROW), P("col"), P(ROW), P("col")),
        check_vma=False,
    )
```

```python
import functools

import jax
import jax.numpy as jnp
from jax import lax
from jax.experimental import pallas as pl
from jax.experimental.pallas import tpu as pltpu
from jax.sharding import Mesh
from jax.sharding import PartitionSpec as P


CLIP = 3072
Y, Z, CORE, X = "row_0", "row_1", "row_2", "col"
ROW = (Y, Z, CORE)

QUERY_GRANT, OUTPUT_GRANT = 16, 16
decay_rate = 0.81
epsilon_one = 1e-30


def shift(value, axis, by):
    size = lax.axis_size(axis)
    return lax.ppermute(value, axis, [(i, (i + by) % size) for i in range(size)])


def fetch_slab(left_ref, left_buf, in_sem, runs, slot):
    at = 0
    for start, columns in runs:
        pltpu.make_async_copy(
            left_ref.at[:, pl.ds(pl.multiple_of(start, 128), columns)],
            left_buf.at[slot, :, pl.ds(at, columns)],
            in_sem.at[slot],
        ).start()
        at += columns


def slab_product(left_buf, right_ref, in_sem, slot):
    whole = left_buf.at[slot]
    pltpu.make_async_copy(whole, whole, in_sem.at[slot]).wait()
    product = lax.dot_general(
        left_buf[slot], right_ref[...], (((0,), (0,)), ((), ())), preferred_element_type=jnp.float32
    )
    return product.astype(jnp.bfloat16)


def query_kernel(
    blocks, group, where_ref, left_ref, right_ref, keep_ref, give_ref, left_buf, in_sem, out_buf
):
    core = where_ref[0]
    slots, _, width = left_buf.shape
    pieces = 8 * group // width
    slabs = [(where_ref[1 + k] + s * width) for k in blocks for s in range(pieces)]

    def fetch(i):
        fetch_slab(left_ref, left_buf, in_sem, [(slabs[i], width)], i % slots)

    for i in range(min(slots, len(slabs))):
        fetch(i)
    for b in range(len(blocks)):

        def slab_step(s, carry, b=b):
            i = b * pieces + s
            product = slab_product(left_buf, right_ref, in_sem, lax.rem(i, slots))
            out_buf[pl.ds(pl.multiple_of(s * width, 128), width), :] = product
            for j in range(slots, len(slabs)):

                @pl.when(i + slots == j)
                def _(j=j):
                    fetch(j)

            return carry

        lax.fori_loop(0, pieces, slab_step, 0)

        def split_step(e, carry, b=b):
            entry = where_ref[9 + e]
            mine = pl.multiple_of((2 * entry + core) * group, 16)
            other = pl.multiple_of((2 * entry + 1 - core) * group, 16)
            keep_ref[b, e] = out_buf[pl.ds(mine, group), :]
            give_ref[b, e] = out_buf[pl.ds(other, group), :]
            return carry

        lax.fori_loop(0, 4, split_step, 0)


def output_kernel(
    blocks, group, where_ref, left_ref, right_ref, keep_ref, give_ref, left_buf, in_sem
):
    core = where_ref[0]
    slots = left_buf.shape[0]
    slabs = [
        [(where_ref[13 + e] * (8 * group) + where_ref[5 + k] + half * group, group) for e in range(4)]
        for k in blocks
        for half in (1 - core, core)
    ]
    for i in range(min(slots, len(slabs))):
        fetch_slab(left_ref, left_buf, in_sem, slabs[i], i % slots)
    for i in range(len(slabs)):
        product = slab_product(left_buf, right_ref, in_sem, i % slots)
        target = keep_ref if i % 2 else give_ref
        target[i // 2] = product.reshape(4, group, product.shape[-1])
        if i + slots < len(slabs):
            fetch_slab(left_ref, left_buf, in_sem, slabs[i + slots], i % slots)


def partial_blocks(where, left, right, blocks, group, aligned, vmem):
    tokens, columns = right.shape
    shape = jax.ShapeDtypeStruct((len(blocks), 4, group, columns), jnp.bfloat16)
    rows = 8 * group
    width = rows // 2 if aligned else rows // 3
    scratch = [pltpu.VMEM((3, tokens, width), jnp.bfloat16), pltpu.SemaphoreType.DMA((3,))]
    if not aligned:
        scratch.append(pltpu.VMEM((rows, columns), jnp.bfloat16))
    return pl.pallas_call(
        functools.partial(output_kernel if aligned else query_kernel, blocks, group),
        out_shape=[shape, shape],
        in_specs=[
            pl.BlockSpec(memory_space=pltpu.SMEM),
            pl.BlockSpec(memory_space=pl.ANY),
            pl.BlockSpec(memory_space=pltpu.VMEM),
        ],
        out_specs=[pl.BlockSpec(memory_space=pltpu.VMEM)] * 2,
        scratch_shapes=scratch,
        compiler_params=pltpu.CompilerParams(vmem_limit_bytes=vmem * 2**20),
        cost_estimate=pl.CostEstimate(
            flops=2 * len(blocks) * rows * tokens * columns,
            bytes_accessed=2 * len(blocks) * rows * tokens,
            transcendentals=0,
        ),
    )(where, left, right)


def add_kernel(plan, step, *refs):
    inputs, outputs = refs[: len(refs) - len(plan)], refs[len(refs) - len(plan) :]
    rows = outputs[0].shape[1]
    for o, entries in enumerate(plan):
        for e, terms in enumerate(entries):

            def chunk(i, carry, o=o, e=e, terms=terms):
                at = pl.ds(pl.multiple_of(i * step, step), step)
                value = None
                for which, entry in terms:
                    term = inputs[which][entry, at, :].astype(jnp.float32)
                    value = term if value is None else value + term
                outputs[o][e, at, :] = value.astype(outputs[o].dtype)
                return carry

            lax.fori_loop(0, rows // step, chunk, 0)


def add_entries(inputs, plan, dtypes=None):
    rows, columns = inputs[0].shape[1:]
    dtypes = dtypes or [jnp.bfloat16] * len(plan)
    return pl.pallas_call(
        functools.partial(add_kernel, plan, 16),
        out_shape=[jax.ShapeDtypeStruct((len(p), rows, columns), d) for p, d in zip(plan, dtypes)],
        in_specs=[pl.BlockSpec(memory_space=pltpu.VMEM)] * len(inputs),
        out_specs=[pl.BlockSpec(memory_space=pltpu.VMEM)] * len(plan),
        cost_estimate=pl.CostEstimate(flops=600_000_000, bytes_accessed=0, transcendentals=0),
        compiler_params=pltpu.CompilerParams(vmem_limit_bytes=12 * 2**20),
    )(*inputs)


def wide(value):
    return value.astype(jnp.float32)


def after(value, *others):
    return lax.optimization_barrier((value, *others))[0]


def flat(value):
    return value.reshape(-1, *value.shape[2:])


def all_sum(value, axis):
    size = lax.axis_size(axis)
    total = value
    for k in range(1, size):
        total = total + shift(value, axis, k)
    return total


def finish(
    gradient, clip_scale, row_old, col_old, row_sums, col_sums, row_level, whole_rows, whole_cols
):
    squared_scale = clip_scale * clip_scale
    row_new = decay_rate * row_old + (1.0 - decay_rate) * (
        squared_scale * row_sums / whole_cols + epsilon_one
    )
    col_new = decay_rate * col_old + (1.0 - decay_rate) * (
        squared_scale * col_sums / whole_rows + epsilon_one
    )
    update = clip_scale * gradient * lax.rsqrt(row_new[:, None] * col_new[None, :] / row_level)
    return (update.astype(jnp.bfloat16), row_new, col_new)


def shards(acts_in, grad_query, attn_out, grad_out, row_query, col_query, row_output, col_output):
    query_rows = row_query.shape[0]
    output_rows = row_output.shape[0]
    query_width = col_query.shape[0]
    output_width = col_output.shape[0]
    y, z, core = lax.axis_index(Y), lax.axis_index(Z), lax.axis_index(CORE)
    pair_query, pair_output = 2 * query_rows, 2 * output_rows
    where = jnp.stack(
        [core]
        + [lax.rem(y + k, 4) * (4 * pair_query) for k in range(4)]
        + [lax.rem(z + k, 4) * pair_output for k in range(4)]
        + [lax.rem(z + k, 4) for k in range(4)]
        + [lax.rem(y + k, 4) for k in range(4)]
    ).astype(jnp.int32)

    def query_blocks(where, ks, vmem):
        kept, give = partial_blocks(where, acts_in, grad_query, ks, query_rows, False, vmem)
        return kept, flat(kept), flat(shift(give, CORE, 1))

    def output_blocks(where, ks, vmem):
        kept, give = partial_blocks(where, attn_out, grad_out, ks, output_rows, True, vmem)
        return kept, flat(kept), flat(shift(give, CORE, 1))

    one, two = (2, 1), (3, 0)
    far_plan = [[[(0, e), (1, e)] for e in half] for half in (one, two)]

    def near_plan(half, relayed, first, third, arrived):
        plan = [[[(i, base + e) for i in which] for e in half] for which, base in (first, third)]
        return [
            [terms + [(arrived, i)] if o == relayed else terms for i, terms in enumerate(entries)]
            for o, entries in enumerate(plan)
        ]

    query_places = (((0, 1), 0), ((0, 1), 4), 2)
    output_places = (((0, 1), 0), ((2, 3), 0), 4)
    last_one = [[[(0, e), (1, e), (2, i), (3, i)]] for i, e in enumerate(one)]
    last_two = [[[(0, e), (1, e), (2, i), (3, i)]] for i, e in enumerate(two)]

    query_made, *query_block = query_blocks(where, (2,), 50)
    output_made, *output_block = output_blocks(after(where, query_made), (2,), 44)
    query_far_one, query_far_two = add_entries(query_block, far_plan)
    query_low = shift(query_far_one, Y, 1)
    query_high = shift(query_far_two, Y, -1)
    output_far_one, output_far_two = add_entries(output_block, far_plan)
    output_low = shift(output_far_one, Z, 1)
    output_high = shift(output_far_two, Z, -1)

    ready = after(where, query_far_one, output_far_one)
    query_made, query_kept, query_got = query_blocks(ready, (1, 3), QUERY_GRANT)
    output_made, *output_1 = output_blocks(after(where, query_made), (1,), OUTPUT_GRANT)
    query_plus_one, query_minus_one = add_entries(
        (query_kept, query_got, query_low), near_plan(one, 0, *query_places)
    )
    query_one = (shift(query_plus_one, Y, 1), shift(query_minus_one, Y, -1))
    output_made, *output_3 = output_blocks(
        after(where, query_plus_one, output_made), (3,), OUTPUT_GRANT
    )
    query_plus_two, query_minus_two = add_entries(
        (query_kept, query_got, query_high), near_plan(two, 1, *query_places)
    )
    query_two = (shift(query_plus_two, Y, 1), shift(query_minus_two, Y, -1))
    output_plus_one, output_minus_one = add_entries(
        (*output_1, *output_3, output_low), near_plan(one, 0, *output_places)
    )
    output_one = (shift(output_plus_one, Z, 1), shift(output_minus_one, Z, -1))
    output_plus_two, output_minus_two = add_entries(
        (*output_1, *output_3, output_high), near_plan(two, 1, *output_places)
    )
    output_two = (shift(output_plus_two, Z, 1), shift(output_minus_two, Z, -1))

    ready = after(where, query_plus_two, output_plus_two)
    query_made, *query_block = query_blocks(ready, (0,), QUERY_GRANT)
    output_made, *output_block = output_blocks(after(where, query_made), (0,), OUTPUT_GRANT)
    wide_own = [jnp.bfloat16, jnp.float32]
    query_2, query_1 = add_entries((*query_block, *query_one), last_one)
    query_sent = [shift(query_2, Z, 2), shift(query_1, Z, 1)]
    output_2, output_1 = add_entries((*output_block, *output_one), last_one)
    output_sent = [shift(output_2, Y, 2), shift(output_1, Y, 1)]
    query_3, query_own = add_entries((*query_block, *query_two), last_two, wide_own)
    query_sent.append(shift(query_3, Z, 3))
    output_3, output_own = add_entries((*output_block, *output_two), last_two, wide_own)
    output_sent.append(shift(output_3, Y, 3))
    query_grad = query_own[0] + sum(wide(p[0]) for p in query_sent)
    output_grad = output_own[0] + sum(wide(p[0]) for p in output_sent)

    query_whole_rows = query_rows * lax.axis_size(ROW)
    output_whole_rows = output_rows * lax.axis_size(ROW)
    query_whole_cols = query_width * lax.axis_size(X)
    output_whole_cols = output_width * lax.axis_size(X)
    query_square = query_grad * query_grad
    output_square = output_grad * output_grad
    query_rowsum = jnp.sum(query_square, axis=1)
    output_rowsum = jnp.sum(output_square, axis=1)
    query_colsum = jnp.sum(query_square, axis=0)
    output_colsum = jnp.sum(output_square, axis=0)
    rowsums = all_sum(jnp.concatenate([query_rowsum, output_rowsum]), X)
    query_rowsum, output_rowsum = rowsums[:query_rows], rowsums[query_rows:]
    scalars = jnp.stack(
        [jnp.sum(query_rowsum), jnp.sum(output_rowsum), jnp.sum(row_query), jnp.sum(row_output)]
    )
    sums = jnp.concatenate([query_colsum, output_colsum, scalars])
    sums = jnp.sum(
        lax.all_to_all(
            jnp.broadcast_to(sums[None, None], (lax.axis_size(ROW), 1, sums.shape[0])),
            ROW,
            0,
            0,
            tiled=True,
        ),
        axis=(0, 1),
    )
    query_colsum = sums[:query_width]
    output_colsum = sums[query_width : query_width + output_width]
    query_squares, output_squares, query_oldsum, output_oldsum = (
        sums[query_width + output_width + i] for i in range(4)
    )
    clip_scale = CLIP / jnp.maximum(jnp.sqrt(query_squares + output_squares), jnp.float32(CLIP))
    squared_scale = clip_scale * clip_scale
    query_level = decay_rate * query_oldsum / query_whole_rows + (1.0 - decay_rate) * (
        squared_scale * query_squares / (query_whole_rows * query_whole_cols) + epsilon_one
    )
    output_level = decay_rate * output_oldsum / output_whole_rows + (1.0 - decay_rate) * (
        squared_scale * output_squares / (output_whole_rows * output_whole_cols) + epsilon_one
    )
    update_query, new_row_query, new_col_query = finish(
        query_grad,
        clip_scale,
        row_query,
        col_query,
        query_rowsum,
        query_colsum,
        query_level,
        query_whole_rows,
        query_whole_cols,
    )
    update_output, new_row_output, new_col_output = finish(
        output_grad,
        clip_scale,
        row_output,
        col_output,
        output_rowsum,
        output_colsum,
        output_level,
        output_whole_rows,
        output_whole_cols,
    )
    return (
        update_query,
        update_output,
        new_row_query,
        new_col_query,
        new_row_output,
        new_col_output,
    )


def solution(mesh):
    split = Mesh(
        mesh.devices.reshape(4, 4, 2, mesh.shape[X]), (Y, Z, CORE, X)
    )
    return jax.shard_map(
        shards,
        mesh=split,
        in_specs=(
            P(ROW, None),
            P(ROW, X),
            P(ROW, None),
            P(ROW, X),
            P(ROW),
            P(X),
            P(ROW),
            P(X),
        ),
        out_specs=(P(ROW, X), P(ROW, X), P(ROW), P(X), P(ROW), P(X)),
        check_vma=False,
    )
```

```python
import functools

import jax
import jax.numpy as jnp
from jax import lax
from jax.experimental import pallas as pl
from jax.experimental.pallas import tpu as pltpu
from jax.sharding import Mesh
from jax.sharding import PartitionSpec as P


CLIP = 3072
Y, Z, CORE, X = "row_0", "row_1", "row_2", "col"
ROW = (Y, Z, CORE)

GRANTS = 50, 46, 45, 40, 42, 42
decay_rate = 0.81
epsilon_one = 1e-30


def shift(value, axis, by):
    size = lax.axis_size(axis)
    return lax.ppermute(value, axis, [(i, (i + by) % size) for i in range(size)])


def block_kernel(
    slabs, group, where_ref, left_ref, right_ref, keep_ref, give_ref, left_buf, in_sem, out_buf, out_sem
):
    core = where_ref[0]
    slots, _, width = left_buf.shape
    flat_slabs = [(b, s, runs) for b, (block, _) in enumerate(slabs) for s, runs in enumerate(block)]

    def fetch(i):
        at = 0
        for index, plus, columns in flat_slabs[i][2]:
            start = pl.multiple_of(where_ref[index] + plus, 128)
            pltpu.make_async_copy(
                left_ref.at[:, pl.ds(start, columns)],
                left_buf.at[i % slots, :, pl.ds(at, columns)],
                in_sem.at[i % slots],
            ).start()
            at += columns

    for i in range(min(slots, len(flat_slabs))):
        fetch(i)
    for i, (b, s, _) in enumerate(flat_slabs):
        slot = i % slots
        whole = left_buf.at[slot]
        pltpu.make_async_copy(whole, whole, in_sem.at[slot]).wait()
        product = lax.dot_general(
            left_buf[slot], right_ref[...], (((0,), (0,)), ((), ())), preferred_element_type=jnp.float32
        )
        out_buf[b, pl.ds(s * width, width), :] = product.astype(jnp.bfloat16)
        if i + slots < len(flat_slabs):
            fetch(i + slots)
        for j in range(s * width // group, (s + 1) * width // group):
            moved(group, slabs[b][1], where_ref, core, keep_ref, give_ref, out_buf, out_sem, b, j)
    for b in range(len(slabs)):
        for j in range(8):
            rows = out_buf.at[b, pl.ds(j * group, group), :]
            pltpu.make_async_copy(rows, keep_ref.at[b, j // 2], out_sem.at[b, j]).wait()


def moved(group, first, where_ref, core, keep_ref, give_ref, out_buf, out_sem, b, j):
    rows = out_buf.at[b, pl.ds(j * group, group), :]
    entry = where_ref[first + j // 2]
    for side, target in ((True, keep_ref), (False, give_ref)):

        @pl.when((core == j % 2) == side)
        def _(target=target):
            pltpu.make_async_copy(rows, target.at[b, entry], out_sem.at[b, j]).start()


def partial_blocks(where, left, right, slabs, group, vmem):
    tokens, columns = right.shape
    blocks, rows = len(slabs), 8 * group
    shape = jax.ShapeDtypeStruct((blocks, 4, group, columns), jnp.bfloat16)
    width = rows // len(slabs[0][0])
    return pl.pallas_call(
        functools.partial(block_kernel, slabs, group),
        out_shape=[shape, shape],
        in_specs=[
            pl.BlockSpec(memory_space=pltpu.SMEM),
            pl.BlockSpec(memory_space=pl.ANY),
            pl.BlockSpec(memory_space=pltpu.VMEM),
        ],
        out_specs=[pl.BlockSpec(memory_space=pltpu.VMEM)] * 2,
        scratch_shapes=[
            pltpu.VMEM((3, tokens, width), jnp.bfloat16),
            pltpu.SemaphoreType.DMA((3,)),
            pltpu.VMEM((blocks, rows, columns), jnp.bfloat16),
            pltpu.SemaphoreType.DMA((blocks, 8)),
        ],
        compiler_params=pltpu.CompilerParams(vmem_limit_bytes=vmem * 2**20),
        cost_estimate=pl.CostEstimate(
            flops=2 * blocks * rows * tokens * columns,
            bytes_accessed=2 * blocks * rows * tokens,
            transcendentals=0,
        ),
    )(where, left, right)


def add_kernel(plan, step, *refs):
    inputs, outputs = refs[: len(refs) - len(plan)], refs[len(refs) - len(plan) :]
    rows = outputs[0].shape[1]
    for o, entries in enumerate(plan):
        for e, terms in enumerate(entries):

            def chunk(i, carry, o=o, e=e, terms=terms):
                at = pl.ds(pl.multiple_of(i * step, step), step)
                value = None
                for which, entry in terms:
                    term = inputs[which][entry, at, :].astype(jnp.float32)
                    value = term if value is None else value + term
                outputs[o][e, at, :] = value.astype(outputs[o].dtype)
                return carry

            lax.fori_loop(0, rows // step, chunk, 0)


def add_entries(inputs, plan, dtypes=None):
    rows, columns = inputs[0].shape[1:]
    dtypes = dtypes or [jnp.bfloat16] * len(plan)
    return pl.pallas_call(
        functools.partial(add_kernel, plan, 16),
        out_shape=[jax.ShapeDtypeStruct((len(p), rows, columns), d) for p, d in zip(plan, dtypes)],
        in_specs=[pl.BlockSpec(memory_space=pltpu.VMEM)] * len(inputs),
        out_specs=[pl.BlockSpec(memory_space=pltpu.VMEM)] * len(plan),
        cost_estimate=pl.CostEstimate(flops=600_000_000, bytes_accessed=0, transcendentals=0),
        compiler_params=pltpu.CompilerParams(vmem_limit_bytes=12 * 2**20),
    )(*inputs)


def wide(value):
    return value.astype(jnp.float32)


def after(value, *others):
    return lax.optimization_barrier((value, *others))[0]


def flat(value):
    return value.reshape(-1, *value.shape[2:])


def all_sum(value, axis):
    size = lax.axis_size(axis)
    total = value
    for k in range(1, size):
        total = total + shift(value, axis, k)
    return total


def finish(
    gradient, clip_scale, row_old, col_old, row_sums, col_sums, row_level, whole_rows, whole_cols
):
    squared_scale = clip_scale * clip_scale
    row_new = decay_rate * row_old + (1.0 - decay_rate) * (
        squared_scale * row_sums / whole_cols + epsilon_one
    )
    col_new = decay_rate * col_old + (1.0 - decay_rate) * (
        squared_scale * col_sums / whole_rows + epsilon_one
    )
    update = clip_scale * gradient * lax.rsqrt(row_new[:, None] * col_new[None, :] / row_level)
    return (update.astype(jnp.bfloat16), row_new, col_new)


def shards(acts_in, grad_query, attn_out, grad_out, row_query, col_query, row_output, col_output):
    query_rows = row_query.shape[0]
    output_rows = row_output.shape[0]
    query_width = col_query.shape[0]
    output_width = col_output.shape[0]
    y, z, core = lax.axis_index(Y), lax.axis_index(Z), lax.axis_index(CORE)
    pair_query, pair_output = 2 * query_rows, 2 * output_rows
    where = jnp.stack(
        [core]
        + [lax.rem(y + k, 4) * (4 * pair_query) for k in range(4)]
        + [lax.rem(z + k, 4) * pair_output for k in range(4)]
        + [lax.rem(k + 4 - z, 4) for k in range(4)]
        + [lax.rem(k + 4 - y, 4) for k in range(4)]
    ).astype(jnp.int32)

    def made(where, left, right, slabs, group, vmem):
        kept, give = partial_blocks(where, left, right, slabs, group, vmem)
        return kept, flat(kept), flat(shift(give, CORE, 1))

    def query_blocks(where, ks, vmem):
        third = 8 * query_rows // 3
        slabs = [([[(1 + k, s * third, third)] for s in range(3)], 9) for k in ks]
        return made(where, acts_in, grad_query, slabs, query_rows, vmem)

    def output_blocks(where, ks, vmem):
        run = lambda k, i: (5 + k, i * 4 * pair_output, pair_output)
        slabs = [([[run(k, 0), run(k, 1)], [run(k, 2), run(k, 3)]], 13) for k in ks]
        return made(where, attn_out, grad_out, slabs, output_rows, vmem)

    one, two = (2, 1), (3, 0)
    far_plan = [[[(0, e), (1, e)] for e in half] for half in (one, two)]

    def near_plan(half, relayed):
        plan = [[[(0, base + e), (1, base + e)] for e in half] for base in (0, 4)]
        for i, terms in enumerate(plan[relayed]):
            terms.append((2, i))
        return plan

    last_one = [[[(0, e), (1, e), (2, i), (3, i)]] for i, e in enumerate(one)]
    last_two = [[[(0, e), (1, e), (2, i), (3, i)]] for i, e in enumerate(two)]

    query_made, *query_block = query_blocks(where, (2,), GRANTS[0])
    output_made, *output_block = output_blocks(after(where, query_made), (2,), GRANTS[1])
    query_far_one, query_far_two = add_entries(query_block, far_plan)
    query_low = shift(query_far_one, Y, 1)
    query_high = shift(query_far_two, Y, -1)
    output_far_one, output_far_two = add_entries(output_block, far_plan)
    output_low = shift(output_far_one, Z, 1)
    output_high = shift(output_far_two, Z, -1)

    ready = after(where, query_far_one, output_far_one)
    query_made, *query_block = query_blocks(ready, (1, 3), GRANTS[2])
    output_made, *output_block = output_blocks(after(where, query_made), (1, 3), GRANTS[3])

    def near(block, arrived, half, relayed, axis):
        plus, minus = add_entries((*block, arrived), near_plan(half, relayed))
        return plus, (shift(plus, axis, 1), shift(minus, axis, -1))

    query_plus, query_one = near(query_block, query_low, one, 0, Y)
    output_plus, output_one = near(output_block, output_low, one, 0, Z)
    query_plus, query_two = near(query_block, query_high, two, 1, Y)
    output_plus, output_two = near(output_block, output_high, two, 1, Z)

    ready = after(where, query_plus, output_plus)
    query_made, *query_block = query_blocks(ready, (0,), GRANTS[4])
    output_made, *output_block = output_blocks(after(where, query_made), (0,), GRANTS[5])
    wide_own = [jnp.bfloat16, jnp.float32]
    query_2, query_1 = add_entries((*query_block, *query_one), last_one)
    query_sent = [shift(query_2, Z, 2), shift(query_1, Z, 1)]
    output_2, output_1 = add_entries((*output_block, *output_one), last_one)
    output_sent = [shift(output_2, Y, 2), shift(output_1, Y, 1)]
    query_3, query_own = add_entries((*query_block, *query_two), last_two, wide_own)
    query_sent.append(shift(query_3, Z, 3))
    output_3, output_own = add_entries((*output_block, *output_two), last_two, wide_own)
    output_sent.append(shift(output_3, Y, 3))
    query_grad = query_own[0] + sum(wide(p[0]) for p in query_sent)
    output_grad = output_own[0] + sum(wide(p[0]) for p in output_sent)

    query_whole_rows = query_rows * lax.axis_size(ROW)
    output_whole_rows = output_rows * lax.axis_size(ROW)
    query_whole_cols = query_width * lax.axis_size(X)
    output_whole_cols = output_width * lax.axis_size(X)
    query_square = query_grad * query_grad
    output_square = output_grad * output_grad
    query_rowsum = jnp.sum(query_square, axis=1)
    output_rowsum = jnp.sum(output_square, axis=1)
    query_colsum = jnp.sum(query_square, axis=0)
    output_colsum = jnp.sum(output_square, axis=0)
    rowsums = all_sum(jnp.concatenate([query_rowsum, output_rowsum]), X)
    query_rowsum, output_rowsum = rowsums[:query_rows], rowsums[query_rows:]
    scalars = jnp.stack(
        [jnp.sum(query_rowsum), jnp.sum(output_rowsum), jnp.sum(row_query), jnp.sum(row_output)]
    )
    sums = jnp.concatenate([query_colsum, output_colsum, scalars])
    sums = jnp.sum(
        lax.all_to_all(
            jnp.broadcast_to(sums[None, None], (lax.axis_size(ROW), 1, sums.shape[0])),
            ROW,
            0,
            0,
            tiled=True,
        ),
        axis=(0, 1),
    )
    query_colsum = sums[:query_width]
    output_colsum = sums[query_width : query_width + output_width]
    query_squares, output_squares, query_oldsum, output_oldsum = (
        sums[query_width + output_width + i] for i in range(4)
    )
    clip_scale = CLIP / jnp.maximum(jnp.sqrt(query_squares + output_squares), jnp.float32(CLIP))
    squared_scale = clip_scale * clip_scale
    query_level = decay_rate * query_oldsum / query_whole_rows + (1.0 - decay_rate) * (
        squared_scale * query_squares / (query_whole_rows * query_whole_cols) + epsilon_one
    )
    output_level = decay_rate * output_oldsum / output_whole_rows + (1.0 - decay_rate) * (
        squared_scale * output_squares / (output_whole_rows * output_whole_cols) + epsilon_one
    )
    update_query, new_row_query, new_col_query = finish(
        query_grad,
        clip_scale,
        row_query,
        col_query,
        query_rowsum,
        query_colsum,
        query_level,
        query_whole_rows,
        query_whole_cols,
    )
    update_output, new_row_output, new_col_output = finish(
        output_grad,
        clip_scale,
        row_output,
        col_output,
        output_rowsum,
        output_colsum,
        output_level,
        output_whole_rows,
        output_whole_cols,
    )
    return (
        update_query,
        update_output,
        new_row_query,
        new_col_query,
        new_row_output,
        new_col_output,
    )


def solution(mesh):
    split = Mesh(
        mesh.devices.reshape(4, 4, 2, mesh.shape[X]), (Y, Z, CORE, X)
    )
    return jax.shard_map(
        shards,
        mesh=split,
        in_specs=(
            P(ROW, None),
            P(ROW, X),
            P(ROW, None),
            P(ROW, X),
            P(ROW),
            P(X),
            P(ROW),
            P(X),
        ),
        out_specs=(P(ROW, X), P(ROW, X), P(ROW), P(X), P(ROW), P(X)),
        check_vma=False,
    )
```

```python
import functools

import jax
import jax.numpy as jnp
from jax import lax
from jax.experimental import pallas as pl
from jax.experimental.pallas import tpu as pltpu
from jax.sharding import Mesh
from jax.sharding import PartitionSpec as P


CLIP = 3072
Y, Z, CORE, X = "row_0", "row_1", "row_2", "col"
ROW = (Y, Z, CORE)

GRANTS = 59, 44, 10, 10, 10, 10
decay_rate = 0.81
epsilon_one = 1e-30


def shift(value, axis, by):
    size = lax.axis_size(axis)
    return lax.ppermute(value, axis, [(i, (i + by) % size) for i in range(size)])


def dot_rows(left, right_ref):
    product = lax.dot_general(
        left, right_ref[...], (((0,), (0,)), ((), ())), preferred_element_type=jnp.float32
    )
    return product.astype(jnp.bfloat16)


def query_kernel(first, group, where_ref, left_ref, right_ref, keep_ref, give_ref):
    core = where_ref[0]
    width = 8 * group // 3

    def block(b, carry):
        start = where_ref[1 + first + 2 * b]
        for side in (0, 1):

            @pl.when(core == side)
            def _(side=side):
                for s in range(3):
                    columns = pl.ds(pl.multiple_of(start + s * width, 128), width)
                    product = dot_rows(left_ref[:, columns], right_ref)
                    for j in range(8):
                        low, high = max(j * group, s * width), min((j + 1) * group, (s + 1) * width)
                        if low < high:
                            target = keep_ref if j % 2 == side else give_ref
                            rows = slice(low - j * group, high - j * group)
                            piece = product[low - s * width : high - s * width]
                            target[b, where_ref[9 + j // 2], rows, :] = piece

        return carry

    lax.fori_loop(0, keep_ref.shape[0], block, 0)


def output_kernel(first, group, where_ref, left_ref, right_ref, keep_ref, give_ref):
    core = where_ref[0]

    def block(b, carry):
        start = where_ref[5 + first + 2 * b]
        for half, target in ((1 - core, give_ref), (core, keep_ref)):
            runs = [
                left_ref[
                    :,
                    pl.ds(
                        pl.multiple_of(
                            start + where_ref[13 + e] * (8 * group) + half * group, 128
                        ),
                        group,
                    ),
                ]
                for e in range(4)
            ]
            product = dot_rows(jnp.concatenate(runs, axis=1), right_ref)
            for e in range(4):
                target[b, e] = product[e * group : (e + 1) * group]
        return carry

    lax.fori_loop(0, keep_ref.shape[0], block, 0)


def first_kernel(
    aligned, first, group, where_ref, left_ref, right_ref,
    keep_ref, give_ref, left_copy, right_copy, total, sem,
):
    core = where_ref[0]
    steps = sem.shape[0] - 1
    tokens = left_ref.shape[0] // steps
    pieces, width = total.shape[:2]
    runs = [pl.ds(i * tokens, tokens) for i in range(steps)]
    loads = [pltpu.make_async_copy(right_ref, right_copy, sem.at[steps])]
    loads += [
        pltpu.make_async_copy(left_ref.at[run], left_copy.at[run], sem.at[i])
        for i, run in enumerate(runs)
    ]
    for load in loads:
        load.start()
    loads[0].wait()
    start = where_ref[(5 if aligned else 1) + first]
    for i, run in enumerate(runs):
        loads[1 + i].wait()

        def slab(s, carry, i=i, run=run):
            if aligned:
                half = lax.rem(1 - core + s, 2)
                starts = [start + where_ref[13 + e] * (8 * group) + half * group for e in range(4)]
            else:
                starts = [start + s * width]
            part = width // len(starts)
            left = [left_copy[run, pl.ds(pl.multiple_of(c, 128), part)] for c in starts]
            product = lax.dot_general(
                left[0] if len(left) == 1 else jnp.concatenate(left, axis=1),
                right_copy[run, :],
                (((0,), (0,)), ((), ())),
                preferred_element_type=jnp.float32,
            )
            total[s] = product if i == 0 else total[s] + product
            return carry

        lax.fori_loop(0, pieces, slab, 0)
    if aligned:
        for e in range(4):
            rows = slice(e * group, (e + 1) * group)
            give_ref[0, e] = total[0, rows].astype(jnp.bfloat16)
            keep_ref[0, e] = total[1, rows].astype(jnp.bfloat16)
        return
    for side in (0, 1):

        @pl.when(core == side)
        def _(side=side):
            for s in range(pieces):
                for j in range(8):
                    low, high = max(j * group, s * width), min((j + 1) * group, (s + 1) * width)
                    if low < high:
                        target = keep_ref if j % 2 == side else give_ref
                        rows = slice(low - j * group, high - j * group)
                        piece = total[s, low - s * width : high - s * width]
                        target[0, where_ref[9 + j // 2], rows, :] = piece.astype(jnp.bfloat16)


def first_blocks(aligned, where, left, right, first, group, vmem):
    tokens, columns = right.shape
    shape = jax.ShapeDtypeStruct((1, 4, group, columns), jnp.bfloat16)
    pieces = 2 if aligned else 3
    return pl.pallas_call(
        functools.partial(first_kernel, aligned, first, group),
        out_shape=[shape, shape],
        in_specs=[pl.BlockSpec(memory_space=pltpu.SMEM)]
        + [pl.BlockSpec(memory_space=pl.ANY)] * 2,
        out_specs=[pl.BlockSpec(memory_space=pltpu.VMEM)] * 2,
        scratch_shapes=[
            pltpu.VMEM(left.shape, left.dtype),
            pltpu.VMEM(right.shape, right.dtype),
            pltpu.VMEM((pieces, 8 * group // pieces, columns), jnp.float32),
            pltpu.SemaphoreType.DMA((5,)),
        ],
        compiler_params=pltpu.CompilerParams(vmem_limit_bytes=vmem * 2**20),
        cost_estimate=pl.CostEstimate(
            flops=16 * group * tokens * columns, bytes_accessed=16 * group * tokens, transcendentals=0
        ),
    )(where, left, right)


def partial_blocks(kernel, where, left, right, blocks, group, vmem):
    tokens, columns = right.shape
    shape = jax.ShapeDtypeStruct((len(blocks), 4, group, columns), jnp.bfloat16)
    rows = 8 * group * len(blocks)
    return pl.pallas_call(
        functools.partial(kernel, blocks[0], group),
        out_shape=[shape, shape],
        in_specs=[pl.BlockSpec(memory_space=pltpu.SMEM)]
        + [pl.BlockSpec(memory_space=pltpu.VMEM)] * 2,
        out_specs=[pl.BlockSpec(memory_space=pltpu.VMEM)] * 2,
        compiler_params=pltpu.CompilerParams(vmem_limit_bytes=vmem * 2**20),
        cost_estimate=pl.CostEstimate(
            flops=2 * rows * tokens * columns, bytes_accessed=2 * rows * tokens, transcendentals=0
        ),
    )(where, left, right)


def add_kernel(plan, step, *refs):
    inputs, outputs = refs[: len(refs) - len(plan)], refs[len(refs) - len(plan) :]
    rows = outputs[0].shape[1]
    for o, entries in enumerate(plan):
        for e, terms in enumerate(entries):

            def chunk(i, carry, o=o, e=e, terms=terms):
                at = pl.ds(pl.multiple_of(i * step, step), step)
                value = None
                for which, entry in terms:
                    term = inputs[which][entry, at, :].astype(jnp.float32)
                    value = term if value is None else value + term
                outputs[o][e, at, :] = value.astype(outputs[o].dtype)
                return carry

            lax.fori_loop(0, rows // step, chunk, 0)


def add_entries(inputs, plan, dtypes=None):
    rows, columns = inputs[0].shape[1:]
    dtypes = dtypes or [jnp.bfloat16] * len(plan)
    return pl.pallas_call(
        functools.partial(add_kernel, plan, 16),
        out_shape=[jax.ShapeDtypeStruct((len(p), rows, columns), d) for p, d in zip(plan, dtypes)],
        in_specs=[pl.BlockSpec(memory_space=pltpu.VMEM)] * len(inputs),
        out_specs=[pl.BlockSpec(memory_space=pltpu.VMEM)] * len(plan),
        cost_estimate=pl.CostEstimate(flops=600_000_000, bytes_accessed=0, transcendentals=0),
        compiler_params=pltpu.CompilerParams(vmem_limit_bytes=12 * 2**20),
    )(*inputs)


def wide(value):
    return value.astype(jnp.float32)


def after(value, *others):
    return lax.optimization_barrier((value, *others))[0]


def flat(value):
    return value.reshape(-1, *value.shape[2:])


def sums_of(gradient):
    square = gradient * gradient
    return jnp.sum(square, axis=1), jnp.sum(square, axis=0)


def pack_kernel(split, *refs):
    rows_refs, (query_cols, output_cols, query_old, output_old, rows_ref, packed_ref) = refs[:4], refs[4:]
    total = rows_refs[0][...] + rows_refs[1][...] + rows_refs[2][...] + rows_refs[3][...]
    rows_ref[...] = total
    lane = lax.broadcasted_iota(jnp.int32, (1, 128), 1)
    scalars = jnp.zeros((1, 128), jnp.float32)
    parts = (total[:, :split], total[:, split:], query_old[...], output_old[...])
    for i, part in enumerate(parts):
        scalars = jnp.where(lane == i, jnp.sum(part, axis=1, keepdims=True), scalars)
    row = jnp.concatenate([query_cols[...], output_cols[...], scalars], axis=1)
    for i in range(packed_ref.shape[0]):
        packed_ref[i] = row


def finish_kernel(
    split,
    across,
    along,
    sums_ref,
    rows_ref,
    query_row,
    query_col,
    output_row,
    output_col,
    query_grad,
    output_grad,
    query_update,
    query_row_new,
    query_col_new,
    output_update,
    output_row_new,
    output_col_new,
):
    sums = sums_ref[0]
    for i in range(1, sums_ref.shape[0]):
        sums = sums + sums_ref[i]
    query_width, output_width = query_col.shape[1], output_col.shape[1]
    lane = lax.broadcasted_iota(jnp.int32, (1, 128), 1)
    tail = sums[:, query_width + output_width :]
    query_squares, output_squares, query_old, output_old = (
        jnp.sum(jnp.where(lane == i, tail, 0.0), axis=1, keepdims=True) for i in range(4)
    )
    norm = jnp.sqrt(query_squares + output_squares)
    clip_scale = CLIP / jnp.maximum(norm, jnp.float32(CLIP))
    squared_scale = clip_scale * clip_scale

    def one(at, offset, squares, old, row, col, grad, update, row_new, col_new):
        rows, columns = grad.shape
        whole_rows, whole_cols = rows * along, columns * across
        fresh = 1.0 - decay_rate

        def mean(value, count):
            return squared_scale * value / count + epsilon_one

        level = decay_rate * old / whole_rows + fresh * mean(squares, whole_rows * whole_cols)
        row_next = decay_rate * row[...] + fresh * mean(rows_ref[:, at : at + rows], whole_cols)
        col_next = decay_rate * col[...] + fresh * mean(sums[:, offset : offset + columns], whole_rows)
        row_new[...] = row_next
        col_new[...] = col_next
        square = (rows, rows)
        diagonal = lax.broadcasted_iota(jnp.int32, square, 0) == lax.broadcasted_iota(
            jnp.int32, square, 1
        )
        down = jnp.sum(jnp.where(diagonal, row_next, 0.0), axis=1, keepdims=True)
        scale = clip_scale * lax.rsqrt(down / level)
        update[...] = (grad[...] * scale * lax.rsqrt(col_next)).astype(jnp.bfloat16)

    one(
        0, 0, query_squares, query_old,
        query_row, query_col, query_grad, query_update, query_row_new, query_col_new,
    )
    one(
        split, query_width, output_squares, output_old,
        output_row, output_col, output_grad, output_update, output_row_new, output_col_new,
    )


def small_call(kernel, outs, *inputs):
    return pl.pallas_call(
        kernel,
        out_shape=[jax.ShapeDtypeStruct(shape, dtype) for shape, dtype in outs],
        in_specs=[pl.BlockSpec(memory_space=pltpu.VMEM)] * len(inputs),
        out_specs=[pl.BlockSpec(memory_space=pltpu.VMEM)] * len(outs),
        compiler_params=pltpu.CompilerParams(vmem_limit_bytes=12 * 2**20),
        cost_estimate=pl.CostEstimate(flops=600_000_000, bytes_accessed=0, transcendentals=0),
    )(*inputs)


def shards(acts_in, grad_query, attn_out, grad_out, row_query, col_query, row_output, col_output):
    query_rows = row_query.shape[0]
    output_rows = row_output.shape[0]
    query_width = col_query.shape[0]
    output_width = col_output.shape[0]
    y, z, core = lax.axis_index(Y), lax.axis_index(Z), lax.axis_index(CORE)
    pair_query, pair_output = 2 * query_rows, 2 * output_rows
    where = jnp.stack(
        [core]
        + [lax.rem(y + k, 4) * (4 * pair_query) for k in range(4)]
        + [lax.rem(z + k, 4) * pair_output for k in range(4)]
        + [lax.rem(k + 4 - z, 4) for k in range(4)]
        + [lax.rem(y + k, 4) for k in range(4)]
    ).astype(jnp.int32)

    def made(kernel, where, left, right, ks, group, vmem):
        kept, give = partial_blocks(kernel, where, left, right, ks, group, vmem)
        return kept, flat(kept), flat(shift(give, CORE, 1))

    def query_blocks(where, ks, vmem):
        return made(query_kernel, where, acts_in, grad_query, ks, query_rows, vmem)

    def output_blocks(where, ks, vmem):
        return made(output_kernel, where, attn_out, grad_out, ks, output_rows, vmem)

    one, two = (2, 1), (3, 0)
    far_plan = [[[(0, e), (1, e)] for e in half] for half in (one, two)]

    def near_plan(half, relayed):
        plan = [[[(0, base + e), (1, base + e)] for e in half] for base in (0, 4)]
        for i, terms in enumerate(plan[relayed]):
            terms.append((2, i))
        return plan

    last_one = [[[(0, e), (1, e), (2, i), (3, i)]] for i, e in enumerate(one)]
    last_two = [[[(0, e), (1, e), (2, i), (3, i)]] for i, e in enumerate(two)]

    keep, give = first_blocks(False, where, acts_in, grad_query, 2, query_rows, GRANTS[0])
    query_block = flat(keep), flat(shift(give, CORE, 1))
    keep, give = first_blocks(
        True, after(where, keep), attn_out, grad_out, 2, output_rows, GRANTS[1]
    )
    output_block = flat(keep), flat(shift(give, CORE, 1))
    query_far_one, query_far_two = add_entries(query_block, far_plan)
    query_low = shift(query_far_one, Y, 1)
    query_high = shift(query_far_two, Y, -1)
    output_far_one, output_far_two = add_entries(output_block, far_plan)
    output_low = shift(output_far_one, Z, 1)
    output_high = shift(output_far_two, Z, -1)

    ready = after(where, query_far_one, output_far_one)
    query_made, *query_block = query_blocks(ready, (1, 3), GRANTS[2])
    output_made, *output_block = output_blocks(after(where, query_made), (1, 3), GRANTS[3])

    def near(block, arrived, half, relayed, axis):
        plus, minus = add_entries((*block, arrived), near_plan(half, relayed))
        return plus, (shift(plus, axis, 1), shift(minus, axis, -1))

    query_plus, query_one = near(query_block, query_low, one, 0, Y)
    output_plus, output_one = near(output_block, output_low, one, 0, Z)
    query_plus, query_two = near(query_block, query_high, two, 1, Y)
    output_plus, output_two = near(output_block, output_high, two, 1, Z)

    ready = after(where, query_plus, output_plus)
    query_made, *query_block = query_blocks(ready, (0,), GRANTS[4])
    output_made, *output_block = output_blocks(after(where, query_made), (0,), GRANTS[5])
    wide_own = [jnp.bfloat16, jnp.float32]
    query_2, query_1 = add_entries((*query_block, *query_one), last_one)
    query_sent = [shift(query_2, Z, 2), shift(query_1, Z, 1)]
    output_2, output_1 = add_entries((*output_block, *output_one), last_one)
    output_sent = [shift(output_2, Y, 2), shift(output_1, Y, 1)]
    query_3, query_own = add_entries((*query_block, *query_two), last_two, wide_own)
    query_sent.append(shift(query_3, Z, 3))
    output_3, output_own = add_entries((*output_block, *output_two), last_two, wide_own)
    output_sent.append(shift(output_3, Y, 3))
    query_grad = query_own[0] + sum(wide(p[0]) for p in query_sent)
    output_grad = output_own[0] + sum(wide(p[0]) for p in output_sent)

    query_rowsum, query_colsum = sums_of(query_grad)
    output_rowsum, output_colsum = sums_of(output_grad)
    line = lambda value: value.reshape(1, -1)
    split = -(-query_rows // 128) * 128
    rows = line(
        jnp.concatenate(
            [query_rowsum, jnp.zeros((split - query_rows,), jnp.float32), output_rowsum]
        )
    )
    others = [shift(rows, X, k) for k in (2, 1, 3)]
    width = query_width + output_width + 128
    rows, packed = small_call(
        functools.partial(pack_kernel, split),
        [(rows.shape, jnp.float32), ((lax.axis_size(ROW), 1, width), jnp.float32)],
        rows,
        *others,
        *(line(v) for v in (query_colsum, output_colsum, row_query, row_output)),
    )
    packed = lax.all_to_all(packed, ROW, 0, 0, tiled=True)
    olds = [line(v) for v in (row_query, col_query, row_output, col_output)]
    update_query, new_row_query, new_col_query, update_output, new_row_output, new_col_output = small_call(
        functools.partial(finish_kernel, split, lax.axis_size(X), lax.axis_size(ROW)),
        [
            (query_grad.shape, jnp.bfloat16),
            (olds[0].shape, jnp.float32),
            (olds[1].shape, jnp.float32),
            (output_grad.shape, jnp.bfloat16),
            (olds[2].shape, jnp.float32),
            (olds[3].shape, jnp.float32),
        ],
        packed,
        rows,
        *olds,
        query_grad,
        output_grad,
    )
    return (
        update_query,
        update_output,
        new_row_query.reshape(-1),
        new_col_query.reshape(-1),
        new_row_output.reshape(-1),
        new_col_output.reshape(-1),
    )


def solution(mesh):
    split = Mesh(
        mesh.devices.reshape(4, 4, 2, mesh.shape[X]), (Y, Z, CORE, X)
    )
    return jax.shard_map(
        shards,
        mesh=split,
        in_specs=(
            P(ROW, None),
            P(ROW, X),
            P(ROW, None),
            P(ROW, X),
            P(ROW),
            P(X),
            P(ROW),
            P(X),
        ),
        out_specs=(P(ROW, X), P(ROW, X), P(ROW), P(X), P(ROW), P(X)),
        check_vma=False,
    )
```

```python
import functools

import jax
import jax.numpy as jnp
from jax import lax
from jax.experimental import pallas as pl
from jax.experimental.pallas import tpu as pltpu
from jax.sharding import Mesh
from jax.sharding import PartitionSpec as P


CLIP = 3072
Y, Z, CORE, X = "row_0", "row_1", "row_2", "col"
ROW = (Y, Z, CORE)

GRANTS = 30, 30, 12, 12, 12, 12
decay_rate = 0.81
epsilon_one = 1e-30


def shift(value, axis, by):
    size = lax.axis_size(axis)
    return lax.ppermute(value, axis, [(i, (i + by) % size) for i in range(size)])


def dot_rows(left, right_ref):
    product = lax.dot_general(
        left, right_ref[...], (((0,), (0,)), ((), ())), preferred_element_type=jnp.float32
    )
    return product.astype(jnp.bfloat16)


def query_kernel(first, group, where_ref, left_ref, right_ref, keep_ref, give_ref):
    core = where_ref[0]
    width = 8 * group // 3

    def block(b, carry):
        start = where_ref[1 + first + 2 * b]
        for side in (0, 1):

            @pl.when(core == side)
            def _(side=side):
                for s in range(3):
                    columns = pl.ds(pl.multiple_of(start + s * width, 128), width)
                    product = dot_rows(left_ref[:, columns], right_ref)
                    for j in range(8):
                        low, high = max(j * group, s * width), min((j + 1) * group, (s + 1) * width)
                        if low < high:
                            target = keep_ref if j % 2 == side else give_ref
                            rows = slice(low - j * group, high - j * group)
                            piece = product[low - s * width : high - s * width]
                            target[b, where_ref[9 + j // 2], rows, :] = piece

        return carry

    lax.fori_loop(0, keep_ref.shape[0], block, 0)


def output_kernel(first, group, where_ref, left_ref, right_ref, keep_ref, give_ref):
    core = where_ref[0]

    def block(b, carry):
        start = where_ref[5 + first + 2 * b]
        for half, target in ((1 - core, give_ref), (core, keep_ref)):
            runs = [
                left_ref[
                    :,
                    pl.ds(
                        pl.multiple_of(
                            start + where_ref[13 + e] * (8 * group) + half * group, 128
                        ),
                        group,
                    ),
                ]
                for e in range(4)
            ]
            product = dot_rows(jnp.concatenate(runs, axis=1), right_ref)
            for e in range(4):
                target[b, e] = product[e * group : (e + 1) * group]
        return carry

    lax.fori_loop(0, keep_ref.shape[0], block, 0)


def partial_blocks(kernel, where, left, right, blocks, group, vmem):
    tokens, columns = right.shape
    shape = jax.ShapeDtypeStruct((len(blocks), 4, group, columns), jnp.bfloat16)
    rows = 8 * group * len(blocks)
    return pl.pallas_call(
        functools.partial(kernel, blocks[0], group),
        out_shape=[shape, shape],
        in_specs=[pl.BlockSpec(memory_space=pltpu.SMEM)]
        + [pl.BlockSpec(memory_space=pltpu.VMEM)] * 2,
        out_specs=[pl.BlockSpec(memory_space=pltpu.VMEM)] * 2,
        compiler_params=pltpu.CompilerParams(vmem_limit_bytes=vmem * 2**20),
        cost_estimate=pl.CostEstimate(
            flops=2 * rows * tokens * columns, bytes_accessed=2 * rows * tokens, transcendentals=0
        ),
    )(where, left, right)


def add_kernel(plan, step, *refs):
    inputs, outputs = refs[: len(refs) - len(plan)], refs[len(refs) - len(plan) :]
    rows = outputs[0].shape[1]
    for o, entries in enumerate(plan):
        for e, terms in enumerate(entries):

            def chunk(i, carry, o=o, e=e, terms=terms):
                at = pl.ds(pl.multiple_of(i * step, step), step)
                value = None
                for which, entry in terms:
                    term = inputs[which][entry, at, :].astype(jnp.float32)
                    value = term if value is None else value + term
                outputs[o][e, at, :] = value.astype(outputs[o].dtype)
                return carry

            lax.fori_loop(0, rows // step, chunk, 0)


def add_entries(inputs, plan, dtypes=None):
    rows, columns = inputs[0].shape[1:]
    dtypes = dtypes or [jnp.bfloat16] * len(plan)
    return pl.pallas_call(
        functools.partial(add_kernel, plan, 16),
        out_shape=[jax.ShapeDtypeStruct((len(p), rows, columns), d) for p, d in zip(plan, dtypes)],
        in_specs=[pl.BlockSpec(memory_space=pltpu.VMEM)] * len(inputs),
        out_specs=[pl.BlockSpec(memory_space=pltpu.VMEM)] * len(plan),
        cost_estimate=pl.CostEstimate(flops=600_000_000, bytes_accessed=0, transcendentals=0),
        compiler_params=pltpu.CompilerParams(vmem_limit_bytes=12 * 2**20),
    )(*inputs)


def wide(value):
    return value.astype(jnp.float32)


def after(value, *others):
    return lax.optimization_barrier((value, *others))[0]


def flat(value):
    return value.reshape(-1, *value.shape[2:])


def sums_of(gradient):
    square = gradient * gradient
    return jnp.sum(square, axis=1), jnp.sum(square, axis=0)


def pack_kernel(split, *refs):
    rows_refs, (query_cols, output_cols, query_old, output_old, rows_ref, packed_ref) = refs[:4], refs[4:]
    total = rows_refs[0][...] + rows_refs[1][...] + rows_refs[2][...] + rows_refs[3][...]
    rows_ref[...] = total
    lane = lax.broadcasted_iota(jnp.int32, (1, 128), 1)
    scalars = jnp.zeros((1, 128), jnp.float32)
    parts = (total[:, :split], total[:, split:], query_old[...], output_old[...])
    for i, part in enumerate(parts):
        scalars = jnp.where(lane == i, jnp.sum(part, axis=1, keepdims=True), scalars)
    row = jnp.concatenate([query_cols[...], output_cols[...], scalars], axis=1)
    for i in range(packed_ref.shape[0]):
        packed_ref[i] = row


def finish_kernel(
    split,
    across,
    along,
    sums_ref,
    rows_ref,
    query_row,
    query_col,
    output_row,
    output_col,
    query_grad,
    output_grad,
    query_update,
    query_row_new,
    query_col_new,
    output_update,
    output_row_new,
    output_col_new,
):
    sums = sums_ref[0]
    for i in range(1, sums_ref.shape[0]):
        sums = sums + sums_ref[i]
    query_width, output_width = query_col.shape[1], output_col.shape[1]
    lane = lax.broadcasted_iota(jnp.int32, (1, 128), 1)
    tail = sums[:, query_width + output_width :]
    query_squares, output_squares, query_old, output_old = (
        jnp.sum(jnp.where(lane == i, tail, 0.0), axis=1, keepdims=True) for i in range(4)
    )
    norm = jnp.sqrt(query_squares + output_squares)
    clip_scale = CLIP / jnp.maximum(norm, jnp.float32(CLIP))
    squared_scale = clip_scale * clip_scale

    def one(at, offset, squares, old, row, col, grad, update, row_new, col_new):
        rows, columns = grad.shape
        whole_rows, whole_cols = rows * along, columns * across
        fresh = 1.0 - decay_rate

        def mean(value, count):
            return squared_scale * value / count + epsilon_one

        level = decay_rate * old / whole_rows + fresh * mean(squares, whole_rows * whole_cols)
        row_next = decay_rate * row[...] + fresh * mean(rows_ref[:, at : at + rows], whole_cols)
        col_next = decay_rate * col[...] + fresh * mean(sums[:, offset : offset + columns], whole_rows)
        row_new[...] = row_next
        col_new[...] = col_next
        square = (rows, rows)
        diagonal = lax.broadcasted_iota(jnp.int32, square, 0) == lax.broadcasted_iota(
            jnp.int32, square, 1
        )
        down = jnp.sum(jnp.where(diagonal, row_next, 0.0), axis=1, keepdims=True)
        scale = clip_scale * lax.rsqrt(down / level)
        update[...] = (grad[...] * scale * lax.rsqrt(col_next)).astype(jnp.bfloat16)

    one(
        0, 0, query_squares, query_old,
        query_row, query_col, query_grad, query_update, query_row_new, query_col_new,
    )
    one(
        split, query_width, output_squares, output_old,
        output_row, output_col, output_grad, output_update, output_row_new, output_col_new,
    )


def small_call(kernel, outs, *inputs):
    return pl.pallas_call(
        kernel,
        out_shape=[jax.ShapeDtypeStruct(shape, dtype) for shape, dtype in outs],
        in_specs=[pl.BlockSpec(memory_space=pltpu.VMEM)] * len(inputs),
        out_specs=[pl.BlockSpec(memory_space=pltpu.VMEM)] * len(outs),
        compiler_params=pltpu.CompilerParams(vmem_limit_bytes=12 * 2**20),
        cost_estimate=pl.CostEstimate(flops=600_000_000, bytes_accessed=0, transcendentals=0),
    )(*inputs)


def shards(acts_in, grad_query, attn_out, grad_out, row_query, col_query, row_output, col_output):
    query_rows = row_query.shape[0]
    output_rows = row_output.shape[0]
    query_width = col_query.shape[0]
    output_width = col_output.shape[0]
    y, z, core = lax.axis_index(Y), lax.axis_index(Z), lax.axis_index(CORE)
    pair_query, pair_output = 2 * query_rows, 2 * output_rows
    where = jnp.stack(
        [core]
        + [lax.rem(y + k, 4) * (4 * pair_query) for k in range(4)]
        + [lax.rem(z + k, 4) * pair_output for k in range(4)]
        + [lax.rem(k + 4 - z, 4) for k in range(4)]
        + [lax.rem(y + k, 4) for k in range(4)]
    ).astype(jnp.int32)

    def made(kernel, where, left, right, ks, group, vmem):
        kept, give = partial_blocks(kernel, where, left, right, ks, group, vmem)
        return kept, flat(kept), flat(shift(give, CORE, 1))

    def query_blocks(where, ks, vmem):
        return made(query_kernel, where, acts_in, grad_query, ks, query_rows, vmem)

    def output_blocks(where, ks, vmem):
        return made(output_kernel, where, attn_out, grad_out, ks, output_rows, vmem)

    one, two = (2, 1), (3, 0)
    far_plan = [[[(0, e), (1, e)] for e in half] for half in (one, two)]

    def near_plan(half, relayed):
        plan = [[[(0, base + e), (1, base + e)] for e in half] for base in (0, 4)]
        for i, terms in enumerate(plan[relayed]):
            terms.append((2, i))
        return plan

    last_one = [[[(0, e), (1, e), (2, i), (3, i)]] for i, e in enumerate(one)]
    last_two = [[[(0, e), (1, e), (2, i), (3, i)]] for i, e in enumerate(two)]

    query_made, *query_block = query_blocks(where, (2,), GRANTS[0])
    output_made, *output_block = output_blocks(after(where, query_made), (2,), GRANTS[1])
    query_far_one, query_far_two = add_entries(query_block, far_plan)
    query_low = shift(query_far_one, Y, 1)
    query_high = shift(query_far_two, Y, -1)
    output_far_one, output_far_two = add_entries(output_block, far_plan)
    output_low = shift(output_far_one, Z, 1)
    output_high = shift(output_far_two, Z, -1)

    ready = after(where, query_far_one, output_far_one)
    query_made, *query_block = query_blocks(ready, (1, 3), GRANTS[2])
    output_made, *output_block = output_blocks(after(where, query_made), (1, 3), GRANTS[3])

    def near(block, arrived, half, relayed, axis):
        plus, minus = add_entries((*block, arrived), near_plan(half, relayed))
        return plus, (shift(plus, axis, 1), shift(minus, axis, -1))

    query_plus, query_one = near(query_block, query_low, one, 0, Y)
    output_plus, output_one = near(output_block, output_low, one, 0, Z)
    query_plus, query_two = near(query_block, query_high, two, 1, Y)
    output_plus, output_two = near(output_block, output_high, two, 1, Z)

    ready = after(where, query_plus, output_plus)
    output_made, *output_block = output_blocks(ready, (0,), GRANTS[4])
    query_made, *query_block = query_blocks(after(where, output_made), (0,), GRANTS[5])
    wide_own = [jnp.bfloat16, jnp.float32]
    query_2, query_1 = add_entries((*query_block, *query_one), last_one)
    query_sent = [shift(query_2, Z, 2), shift(query_1, Z, 1)]
    output_2, output_1 = add_entries((*output_block, *output_one), last_one)
    output_sent = [shift(output_2, Y, 2), shift(output_1, Y, 1)]
    query_3, query_own = add_entries((*query_block, *query_two), last_two, wide_own)
    query_sent.append(shift(query_3, Z, 3))
    output_3, output_own = add_entries((*output_block, *output_two), last_two, wide_own)
    output_sent.append(shift(output_3, Y, 3))
    query_grad = query_own[0] + sum(wide(p[0]) for p in query_sent)
    output_grad = output_own[0] + sum(wide(p[0]) for p in output_sent)

    query_rowsum, query_colsum = sums_of(query_grad)
    output_rowsum, output_colsum = sums_of(output_grad)
    line = lambda value: value.reshape(1, -1)
    split = -(-query_rows // 128) * 128
    rows = line(
        jnp.concatenate(
            [query_rowsum, jnp.zeros((split - query_rows,), jnp.float32), output_rowsum]
        )
    )
    others = [shift(rows, X, k) for k in (2, 1, 3)]
    width = query_width + output_width + 128
    rows, packed = small_call(
        functools.partial(pack_kernel, split),
        [(rows.shape, jnp.float32), ((lax.axis_size(ROW), 1, width), jnp.float32)],
        rows,
        *others,
        *(line(v) for v in (query_colsum, output_colsum, row_query, row_output)),
    )
    packed = lax.all_to_all(packed, ROW, 0, 0, tiled=True)
    olds = [line(v) for v in (row_query, col_query, row_output, col_output)]
    update_query, new_row_query, new_col_query, update_output, new_row_output, new_col_output = small_call(
        functools.partial(finish_kernel, split, lax.axis_size(X), lax.axis_size(ROW)),
        [
            (query_grad.shape, jnp.bfloat16),
            (olds[0].shape, jnp.float32),
            (olds[1].shape, jnp.float32),
            (output_grad.shape, jnp.bfloat16),
            (olds[2].shape, jnp.float32),
            (olds[3].shape, jnp.float32),
        ],
        packed,
        rows,
        *olds,
        query_grad,
        output_grad,
    )
    return (
        update_query,
        update_output,
        new_row_query.reshape(-1),
        new_col_query.reshape(-1),
        new_row_output.reshape(-1),
        new_col_output.reshape(-1),
    )


def solution(mesh):
    split = Mesh(
        mesh.devices.reshape(4, 4, 2, mesh.shape[X]), (Y, Z, CORE, X)
    )
    return jax.shard_map(
        shards,
        mesh=split,
        in_specs=(
            P(ROW, None),
            P(ROW, X),
            P(ROW, None),
            P(ROW, X),
            P(ROW),
            P(X),
            P(ROW),
            P(X),
        ),
        out_specs=(P(ROW, X), P(ROW, X), P(ROW), P(X), P(ROW), P(X)),
        check_vma=False,
    )
```

```python
import functools

import jax
import jax.numpy as jnp
from jax import lax
from jax.experimental import pallas as pl
from jax.experimental.pallas import tpu as pltpu
from jax.sharding import Mesh
from jax.sharding import PartitionSpec as P


CLIP = 3072
Y, Z, CORE, X = "row_0", "row_1", "row_2", "col"
ROW = (Y, Z, CORE)

GRANTS = 30, 30, 12, 12, 12, 12
decay_rate = 0.81
epsilon_one = 1e-30


def shift(value, axis, by):
    size = lax.axis_size(axis)
    return lax.ppermute(value, axis, [(i, (i + by) % size) for i in range(size)])


def dot_rows(left, right_ref):
    product = lax.dot_general(
        left, right_ref[...], (((0,), (0,)), ((), ())), preferred_element_type=jnp.float32
    )
    return product.astype(jnp.bfloat16)


def query_kernel(first, group, where_ref, left_ref, right_ref, keep_ref, give_ref):
    core = where_ref[0]
    width = 8 * group // 3

    def block(b, carry):
        start = where_ref[1 + first + 2 * b]
        for side in (0, 1):

            @pl.when(core == side)
            def _(side=side):
                for s in range(3):
                    columns = pl.ds(pl.multiple_of(start + s * width, 128), width)
                    product = dot_rows(left_ref[:, columns], right_ref)
                    for j in range(8):
                        low, high = max(j * group, s * width), min((j + 1) * group, (s + 1) * width)
                        if low < high:
                            target = keep_ref if j % 2 == side else give_ref
                            rows = slice(low - j * group, high - j * group)
                            piece = product[low - s * width : high - s * width]
                            target[b, where_ref[9 + j // 2], rows, :] = piece

        return carry

    lax.fori_loop(0, keep_ref.shape[0], block, 0)


def output_kernel(first, group, where_ref, left_ref, right_ref, keep_ref, give_ref):
    core = where_ref[0]

    def block(b, carry):
        start = where_ref[5 + first + 2 * b]
        for half, target in ((1 - core, give_ref), (core, keep_ref)):
            runs = [
                left_ref[
                    :,
                    pl.ds(
                        pl.multiple_of(
                            start + where_ref[13 + e] * (8 * group) + half * group, 128
                        ),
                        group,
                    ),
                ]
                for e in range(4)
            ]
            product = dot_rows(jnp.concatenate(runs, axis=1), right_ref)
            for e in range(4):
                target[b, e] = product[e * group : (e + 1) * group]
        return carry

    lax.fori_loop(0, keep_ref.shape[0], block, 0)


def partial_blocks(kernel, where, left, right, blocks, group, vmem):
    tokens, columns = right.shape
    shape = jax.ShapeDtypeStruct((len(blocks), 4, group, columns), jnp.bfloat16)
    rows = 8 * group * len(blocks)
    return pl.pallas_call(
        functools.partial(kernel, blocks[0], group),
        out_shape=[shape, shape],
        in_specs=[pl.BlockSpec(memory_space=pltpu.SMEM)]
        + [pl.BlockSpec(memory_space=pltpu.VMEM)] * 2,
        out_specs=[pl.BlockSpec(memory_space=pltpu.VMEM)] * 2,
        compiler_params=pltpu.CompilerParams(vmem_limit_bytes=vmem * 2**20),
        cost_estimate=pl.CostEstimate(
            flops=2 * rows * tokens * columns, bytes_accessed=2 * rows * tokens, transcendentals=0
        ),
    )(where, left, right)


def add_kernel(plan, step, *refs):
    inputs, outputs = refs[: len(refs) - len(plan)], refs[len(refs) - len(plan) :]
    rows = outputs[0].shape[1]
    for o, entries in enumerate(plan):
        for e, terms in enumerate(entries):

            def chunk(i, carry, o=o, e=e, terms=terms):
                at = pl.ds(pl.multiple_of(i * step, step), step)
                value = None
                for which, entry in terms:
                    term = inputs[which][entry, at, :].astype(jnp.float32)
                    value = term if value is None else value + term
                outputs[o][e, at, :] = value.astype(outputs[o].dtype)
                return carry

            lax.fori_loop(0, rows // step, chunk, 0)


def add_entries(inputs, plan, dtypes=None):
    rows, columns = inputs[0].shape[1:]
    dtypes = dtypes or [jnp.bfloat16] * len(plan)
    return pl.pallas_call(
        functools.partial(add_kernel, plan, 16),
        out_shape=[jax.ShapeDtypeStruct((len(p), rows, columns), d) for p, d in zip(plan, dtypes)],
        in_specs=[pl.BlockSpec(memory_space=pltpu.VMEM)] * len(inputs),
        out_specs=[pl.BlockSpec(memory_space=pltpu.VMEM)] * len(plan),
        cost_estimate=pl.CostEstimate(flops=600_000_000, bytes_accessed=0, transcendentals=0),
        compiler_params=pltpu.CompilerParams(vmem_limit_bytes=12 * 2**20),
    )(*inputs)


def wide(value):
    return value.astype(jnp.float32)


def after(value, *others):
    return lax.optimization_barrier((value, *others))[0]


def flat(value):
    return value.reshape(-1, *value.shape[2:])


def sums_of(gradient):
    square = gradient * gradient
    return jnp.sum(square, axis=1), jnp.sum(square, axis=0)


def halves_kernel(split, where_ref, rows, query_cols, output_cols, query_old, output_old, keep_ref, give_ref):
    core = where_ref[0]
    width = keep_ref.shape[1] - 128
    lane = lax.broadcasted_iota(jnp.int32, (1, 128), 1)
    scalars = jnp.zeros((1, 128), jnp.float32)
    parts = (rows[:, :split], rows[:, split:], query_old[...], output_old[...])
    for i, part in enumerate(parts):
        scalars = jnp.where(lane == i, jnp.sum(part, axis=1, keepdims=True), scalars)
    columns = query_cols.shape[1] + output_cols.shape[1]
    pad = jnp.zeros((1, 2 * width - columns), jnp.float32)
    whole = jnp.concatenate([query_cols[...], output_cols[...], pad], axis=1)
    low, high = whole[:, :width], whole[:, width:]
    keep_ref[...] = jnp.concatenate([jnp.where(core == 0, low, high), scalars], axis=1)
    give_ref[...] = jnp.concatenate([jnp.where(core == 0, high, low), scalars], axis=1)


def pack_kernel(keep, got, rows, packed_ref):
    total = keep[...] + got[...]
    width = total.shape[1] - 128
    row = jnp.concatenate([total[:, :width], rows[...], total[:, width:]], axis=1)
    for i in range(packed_ref.shape[0]):
        packed_ref[i] = row


def unpack_kernel(where_ref, packed, half_ref, rows_ref, scalars_ref):
    place, column = where_ref[17], where_ref[18]
    width, length = half_ref.shape[1], rows_ref.shape[1]
    peers = packed.shape[0] // 4
    mine = packed[column]
    for p in range(1, peers):
        mine = mine + packed[4 * p + column]
    rows = packed[4 * place]
    for j in range(1, 4):
        rows = rows + packed[4 * place + j]
    everyone = packed[0, :, width + length :]
    for p in range(1, 4 * peers):
        everyone = everyone + packed[p, :, width + length :]
    lane = lax.broadcasted_iota(jnp.int32, (1, 128), 1)
    half_ref[...] = mine[:, :width]
    rows_ref[...] = rows[:, width : width + length]
    scalars_ref[...] = jnp.where(lane < 2, everyone, mine[:, width + length :])


def finish_kernel(
    split,
    across,
    along,
    where_ref,
    half_ref,
    other_ref,
    scalars_ref,
    rows_ref,
    query_row,
    query_col,
    output_row,
    output_col,
    query_grad,
    output_grad,
    query_update,
    query_row_new,
    query_col_new,
    output_update,
    output_row_new,
    output_col_new,
):
    core = where_ref[0]
    half, other = half_ref[...], other_ref[...]
    first, second = jnp.where(core == 0, half, other), jnp.where(core == 0, other, half)
    sums = jnp.concatenate([first, second], axis=1)
    query_width = query_col.shape[1]
    lane = lax.broadcasted_iota(jnp.int32, (1, 128), 1)
    tail = scalars_ref[...]
    query_squares, output_squares, query_old, output_old = (
        jnp.sum(jnp.where(lane == i, tail, 0.0), axis=1, keepdims=True) for i in range(4)
    )
    norm = jnp.sqrt(query_squares + output_squares)
    clip_scale = CLIP / jnp.maximum(norm, jnp.float32(CLIP))
    squared_scale = clip_scale * clip_scale

    def one(at, offset, squares, old, row, col, grad, update, row_new, col_new):
        rows, columns = grad.shape
        whole_rows, whole_cols = rows * along, columns * across
        fresh = 1.0 - decay_rate

        def mean(value, count):
            return squared_scale * value / count + epsilon_one

        level = decay_rate * old / whole_rows + fresh * mean(squares, whole_rows * whole_cols)
        row_next = decay_rate * row[...] + fresh * mean(rows_ref[:, at : at + rows], whole_cols)
        col_next = decay_rate * col[...] + fresh * mean(sums[:, offset : offset + columns], whole_rows)
        row_new[...] = row_next
        col_new[...] = col_next
        square = (rows, rows)
        diagonal = lax.broadcasted_iota(jnp.int32, square, 0) == lax.broadcasted_iota(
            jnp.int32, square, 1
        )
        down = jnp.sum(jnp.where(diagonal, row_next, 0.0), axis=1, keepdims=True)
        scale = clip_scale * lax.rsqrt(down / level)
        update[...] = (grad[...] * scale * lax.rsqrt(col_next)).astype(jnp.bfloat16)

    one(
        0, 0, query_squares, query_old,
        query_row, query_col, query_grad, query_update, query_row_new, query_col_new,
    )
    one(
        split, query_width, output_squares, output_old,
        output_row, output_col, output_grad, output_update, output_row_new, output_col_new,
    )


def small_call(kernel, outs, *inputs, where=None):
    places = [] if where is None else [pl.BlockSpec(memory_space=pltpu.SMEM)]
    return pl.pallas_call(
        kernel,
        out_shape=[jax.ShapeDtypeStruct(shape, dtype) for shape, dtype in outs],
        in_specs=places + [pl.BlockSpec(memory_space=pltpu.VMEM)] * len(inputs),
        out_specs=[pl.BlockSpec(memory_space=pltpu.VMEM)] * len(outs),
        compiler_params=pltpu.CompilerParams(vmem_limit_bytes=12 * 2**20),
        cost_estimate=pl.CostEstimate(flops=600_000_000, bytes_accessed=0, transcendentals=0),
    )(*([] if where is None else [where]), *inputs)


def shards(acts_in, grad_query, attn_out, grad_out, row_query, col_query, row_output, col_output):
    query_rows = row_query.shape[0]
    output_rows = row_output.shape[0]
    query_width = col_query.shape[0]
    output_width = col_output.shape[0]
    y, z, core = lax.axis_index(Y), lax.axis_index(Z), lax.axis_index(CORE)
    pair_query, pair_output = 2 * query_rows, 2 * output_rows
    where = jnp.stack(
        [core]
        + [lax.rem(y + k, 4) * (4 * pair_query) for k in range(4)]
        + [lax.rem(z + k, 4) * pair_output for k in range(4)]
        + [lax.rem(k + 4 - z, 4) for k in range(4)]
        + [lax.rem(y + k, 4) for k in range(4)]
        + [4 * y + z, lax.axis_index(X)]
    ).astype(jnp.int32)

    def made(kernel, where, left, right, ks, group, vmem):
        kept, give = partial_blocks(kernel, where, left, right, ks, group, vmem)
        return kept, flat(kept), flat(shift(give, CORE, 1))

    def query_blocks(where, ks, vmem):
        return made(query_kernel, where, acts_in, grad_query, ks, query_rows, vmem)

    def output_blocks(where, ks, vmem):
        return made(output_kernel, where, attn_out, grad_out, ks, output_rows, vmem)

    one, two = (2, 1), (3, 0)
    far_plan = [[[(0, e), (1, e)] for e in half] for half in (one, two)]

    def near_plan(half, relayed):
        plan = [[[(0, base + e), (1, base + e)] for e in half] for base in (0, 4)]
        for i, terms in enumerate(plan[relayed]):
            terms.append((2, i))
        return plan

    last_one = [[[(0, e), (1, e), (2, i), (3, i)]] for i, e in enumerate(one)]
    last_two = [[[(0, e), (1, e), (2, i), (3, i)]] for i, e in enumerate(two)]

    query_made, *query_block = query_blocks(where, (2,), GRANTS[0])
    output_made, *output_block = output_blocks(after(where, query_made), (2,), GRANTS[1])
    query_far_one, query_far_two = add_entries(query_block, far_plan)
    query_low = shift(query_far_one, Y, 1)
    query_high = shift(query_far_two, Y, -1)
    output_far_one, output_far_two = add_entries(output_block, far_plan)
    output_low = shift(output_far_one, Z, 1)
    output_high = shift(output_far_two, Z, -1)

    ready = after(where, query_far_one, output_far_one)
    query_made, *query_block = query_blocks(ready, (1, 3), GRANTS[2])
    output_made, *output_block = output_blocks(after(where, query_made), (1, 3), GRANTS[3])

    def near(block, arrived, half, relayed, axis):
        plus, minus = add_entries((*block, arrived), near_plan(half, relayed))
        return plus, (shift(plus, axis, 1), shift(minus, axis, -1))

    query_plus, query_one = near(query_block, query_low, one, 0, Y)
    output_plus, output_one = near(output_block, output_low, one, 0, Z)
    query_plus, query_two = near(query_block, query_high, two, 1, Y)
    output_plus, output_two = near(output_block, output_high, two, 1, Z)

    ready = after(where, query_plus, output_plus)
    output_made, *output_block = output_blocks(ready, (0,), GRANTS[4])
    query_made, *query_block = query_blocks(after(where, output_made), (0,), GRANTS[5])
    wide_own = [jnp.bfloat16, jnp.float32]
    query_2, query_1 = add_entries((*query_block, *query_one), last_one)
    query_sent = [shift(query_2, Z, 2), shift(query_1, Z, 1)]
    output_2, output_1 = add_entries((*output_block, *output_one), last_one)
    output_sent = [shift(output_2, Y, 2), shift(output_1, Y, 1)]
    query_3, query_own = add_entries((*query_block, *query_two), last_two, wide_own)
    query_sent.append(shift(query_3, Z, 3))
    output_3, output_own = add_entries((*output_block, *output_two), last_two, wide_own)
    output_sent.append(shift(output_3, Y, 3))
    query_grad = query_own[0] + sum(wide(p[0]) for p in query_sent)
    output_grad = output_own[0] + sum(wide(p[0]) for p in output_sent)

    query_rowsum, query_colsum = sums_of(query_grad)
    output_rowsum, output_colsum = sums_of(output_grad)
    line = lambda value: value.reshape(1, -1)
    split = -(-query_rows // 128) * 128
    rows = line(
        jnp.concatenate(
            [query_rowsum, jnp.zeros((split - query_rows,), jnp.float32), output_rowsum]
        )
    )
    width = -(-(query_width + output_width) // 256) * 128
    packet = ((1, width + 128), jnp.float32)
    sums = [line(v) for v in (query_colsum, output_colsum, row_query, row_output)]
    keep, give = small_call(
        functools.partial(halves_kernel, split), [packet, packet], rows, *sums, where=where
    )
    got = shift(give, CORE, 1)
    peers = (Y, Z, X)
    count = lax.axis_size(peers)
    (packed,) = small_call(
        pack_kernel, [((count, 1, width + 128 + rows.shape[1]), jnp.float32)], keep, got, rows
    )
    packed = lax.all_to_all(packed, peers, 0, 0, tiled=True)
    half, rows, scalars = small_call(
        unpack_kernel,
        [((1, width), jnp.float32), (rows.shape, jnp.float32), ((1, 128), jnp.float32)],
        packed,
        where=where,
    )
    other = shift(half, CORE, 1)
    olds = [line(v) for v in (row_query, col_query, row_output, col_output)]
    update_query, new_row_query, new_col_query, update_output, new_row_output, new_col_output = small_call(
        functools.partial(finish_kernel, split, lax.axis_size(X), lax.axis_size(ROW)),
        [
            (query_grad.shape, jnp.bfloat16),
            (olds[0].shape, jnp.float32),
            (olds[1].shape, jnp.float32),
            (output_grad.shape, jnp.bfloat16),
            (olds[2].shape, jnp.float32),
            (olds[3].shape, jnp.float32),
        ],
        half,
        other,
        scalars,
        rows,
        *olds,
        query_grad,
        output_grad,
        where=where,
    )
    return (
        update_query,
        update_output,
        new_row_query.reshape(-1),
        new_col_query.reshape(-1),
        new_row_output.reshape(-1),
        new_col_output.reshape(-1),
    )


def solution(mesh):
    split = Mesh(
        mesh.devices.reshape(4, 4, 2, mesh.shape[X]), (Y, Z, CORE, X)
    )
    return jax.shard_map(
        shards,
        mesh=split,
        in_specs=(
            P(ROW, None),
            P(ROW, X),
            P(ROW, None),
            P(ROW, X),
            P(ROW),
            P(X),
            P(ROW),
            P(X),
        ),
        out_specs=(P(ROW, X), P(ROW, X), P(ROW), P(X), P(ROW), P(X)),
        check_vma=False,
    )
```

```python
import functools

import jax
import jax.numpy as jnp
from jax import lax
from jax.experimental import pallas as pl
from jax.experimental.pallas import tpu as pltpu
from jax.sharding import Mesh
from jax.sharding import PartitionSpec as P


CLIP = 3072
Y, Z, CORE, X = "row_0", "row_1", "row_2", "col"
ROW = (Y, Z, CORE)

GRANTS = 30, 30, 12, 12, 12, 12
decay_rate = 0.81
epsilon_one = 1e-30


def shift(value, axis, by):
    size = lax.axis_size(axis)
    return lax.ppermute(value, axis, [(i, (i + by) % size) for i in range(size)])


def dot_rows(left, right_ref):
    product = lax.dot_general(
        left, right_ref[...], (((0,), (0,)), ((), ())), preferred_element_type=jnp.float32
    )
    return product.astype(jnp.bfloat16)


def query_kernel(first, group, where_ref, left_ref, right_ref, keep_ref, give_ref):
    core = where_ref[0]
    width = 8 * group // 3

    def block(b, carry):
        start = where_ref[1 + first + 2 * b]
        for side in (0, 1):

            @pl.when(core == side)
            def _(side=side):
                for s in range(3):
                    columns = pl.ds(pl.multiple_of(start + s * width, 128), width)
                    product = dot_rows(left_ref[:, columns], right_ref)
                    for j in range(8):
                        low, high = max(j * group, s * width), min((j + 1) * group, (s + 1) * width)
                        if low < high:
                            target = keep_ref if j % 2 == side else give_ref
                            rows = slice(low - j * group, high - j * group)
                            piece = product[low - s * width : high - s * width]
                            target[b, where_ref[9 + j // 2], rows, :] = piece

        return carry

    lax.fori_loop(0, keep_ref.shape[0], block, 0)


def output_kernel(first, group, where_ref, left_ref, right_ref, keep_ref, give_ref):
    core = where_ref[0]

    def block(b, carry):
        start = where_ref[5 + first + 2 * b]
        for half, target in ((1 - core, give_ref), (core, keep_ref)):
            runs = [
                left_ref[
                    :,
                    pl.ds(
                        pl.multiple_of(
                            start + where_ref[13 + e] * (8 * group) + half * group, 128
                        ),
                        group,
                    ),
                ]
                for e in range(4)
            ]
            product = dot_rows(jnp.concatenate(runs, axis=1), right_ref)
            for e in range(4):
                target[b, e] = product[e * group : (e + 1) * group]
        return carry

    lax.fori_loop(0, keep_ref.shape[0], block, 0)


def partial_blocks(kernel, where, left, right, blocks, group, vmem):
    tokens, columns = right.shape
    shape = jax.ShapeDtypeStruct((len(blocks), 4, group, columns), jnp.bfloat16)
    rows = 8 * group * len(blocks)
    return pl.pallas_call(
        functools.partial(kernel, blocks[0], group),
        out_shape=[shape, shape],
        in_specs=[pl.BlockSpec(memory_space=pltpu.SMEM)]
        + [pl.BlockSpec(memory_space=pltpu.VMEM)] * 2,
        out_specs=[pl.BlockSpec(memory_space=pltpu.VMEM)] * 2,
        compiler_params=pltpu.CompilerParams(vmem_limit_bytes=vmem * 2**20),
        cost_estimate=pl.CostEstimate(
            flops=2 * rows * tokens * columns, bytes_accessed=2 * rows * tokens, transcendentals=0
        ),
    )(where, left, right)


def add_kernel(plan, step, *refs):
    inputs, outputs = refs[: len(refs) - len(plan)], refs[len(refs) - len(plan) :]
    rows = outputs[0].shape[1]
    for o, entries in enumerate(plan):
        for e, terms in enumerate(entries):

            def chunk(i, carry, o=o, e=e, terms=terms):
                at = pl.ds(pl.multiple_of(i * step, step), step)
                value = None
                for which, entry in terms:
                    term = inputs[which][entry, at, :].astype(jnp.float32)
                    value = term if value is None else value + term
                outputs[o][e, at, :] = value.astype(outputs[o].dtype)
                return carry

            lax.fori_loop(0, rows // step, chunk, 0)


def add_entries(inputs, plan, dtypes=None):
    rows, columns = inputs[0].shape[1:]
    dtypes = dtypes or [jnp.bfloat16] * len(plan)
    return pl.pallas_call(
        functools.partial(add_kernel, plan, 16),
        out_shape=[jax.ShapeDtypeStruct((len(p), rows, columns), d) for p, d in zip(plan, dtypes)],
        in_specs=[pl.BlockSpec(memory_space=pltpu.VMEM)] * len(inputs),
        out_specs=[pl.BlockSpec(memory_space=pltpu.VMEM)] * len(plan),
        cost_estimate=pl.CostEstimate(flops=600_000_000, bytes_accessed=0, transcendentals=0),
        compiler_params=pltpu.CompilerParams(vmem_limit_bytes=12 * 2**20),
    )(*inputs)


def wide(value):
    return value.astype(jnp.float32)


def after(value, *others):
    return lax.optimization_barrier((value, *others))[0]


def flat(value):
    return value.reshape(-1, *value.shape[2:])


def sums_of(gradient):
    square = gradient * gradient
    return jnp.sum(square, axis=1), jnp.sum(square, axis=0)


def halves_kernel(split, where_ref, rows, query_cols, output_cols, query_old, output_old, keep_ref, give_ref):
    core = where_ref[0]
    width = keep_ref.shape[1] - 128
    lane = lax.broadcasted_iota(jnp.int32, (1, 128), 1)
    scalars = jnp.zeros((1, 128), jnp.float32)
    parts = (rows[:, :split], rows[:, split:], query_old[...], output_old[...])
    for i, part in enumerate(parts):
        scalars = jnp.where(lane == i, jnp.sum(part, axis=1, keepdims=True), scalars)
    columns = query_cols.shape[1] + output_cols.shape[1]
    pad = jnp.zeros((1, 2 * width - columns), jnp.float32)
    whole = jnp.concatenate([query_cols[...], output_cols[...], pad], axis=1)
    low, high = whole[:, :width], whole[:, width:]
    keep_ref[...] = jnp.concatenate([jnp.where(core == 0, low, high), scalars], axis=1)
    give_ref[...] = jnp.concatenate([jnp.where(core == 0, high, low), scalars], axis=1)


def exchanged(value, axis):
    return [shift(value, axis, k) for k in (2, 1, 3)]


def four(own, far, near, after):
    return (own + far) + (near + after)


def finish_kernel(
    split,
    across,
    along,
    where_ref,
    half_ref,
    other_ref,
    row_0,
    row_1,
    row_2,
    row_3,
    query_row,
    query_col,
    output_row,
    output_col,
    query_grad,
    output_grad,
    query_update,
    query_row_new,
    query_col_new,
    output_update,
    output_row_new,
    output_col_new,
):
    core = where_ref[0]
    other = other_ref[...]
    half, old = half_ref[:, : other.shape[1]], half_ref[:, other.shape[1] :]
    all_rows = four(row_0[...], row_1[...], row_2[...], row_3[...])
    first, second = jnp.where(core == 0, half, other), jnp.where(core == 0, other, half)
    sums = jnp.concatenate([first, second], axis=1)
    query_width = query_col.shape[1]
    lane = lax.broadcasted_iota(jnp.int32, (1, 128), 1)
    tail = jnp.where(lane < 2, all_rows[:, all_rows.shape[1] - 128 :], old)
    query_squares, output_squares, query_old, output_old = (
        jnp.sum(jnp.where(lane == i, tail, 0.0), axis=1, keepdims=True) for i in range(4)
    )
    norm = jnp.sqrt(query_squares + output_squares)
    clip_scale = CLIP / jnp.maximum(norm, jnp.float32(CLIP))
    squared_scale = clip_scale * clip_scale

    def one(at, offset, squares, old, row, col, grad, update, row_new, col_new):
        rows, columns = grad.shape
        whole_rows, whole_cols = rows * along, columns * across
        fresh = 1.0 - decay_rate

        def mean(value, count):
            return squared_scale * value / count + epsilon_one

        level = decay_rate * old / whole_rows + fresh * mean(squares, whole_rows * whole_cols)
        row_next = decay_rate * row[...] + fresh * mean(all_rows[:, at : at + rows], whole_cols)
        col_next = decay_rate * col[...] + fresh * mean(sums[:, offset : offset + columns], whole_rows)
        row_new[...] = row_next
        col_new[...] = col_next
        square = (rows, rows)
        diagonal = lax.broadcasted_iota(jnp.int32, square, 0) == lax.broadcasted_iota(
            jnp.int32, square, 1
        )
        down = jnp.sum(jnp.where(diagonal, row_next, 0.0), axis=1, keepdims=True)
        scale = clip_scale * lax.rsqrt(down / level)
        update[...] = (grad[...] * scale * lax.rsqrt(col_next)).astype(jnp.bfloat16)

    one(
        0, 0, query_squares, query_old,
        query_row, query_col, query_grad, query_update, query_row_new, query_col_new,
    )
    one(
        split, query_width, output_squares, output_old,
        output_row, output_col, output_grad, output_update, output_row_new, output_col_new,
    )


def small_call(kernel, outs, *inputs, where=None):
    places = [] if where is None else [pl.BlockSpec(memory_space=pltpu.SMEM)]
    return pl.pallas_call(
        kernel,
        out_shape=[jax.ShapeDtypeStruct(shape, dtype) for shape, dtype in outs],
        in_specs=places + [pl.BlockSpec(memory_space=pltpu.VMEM)] * len(inputs),
        out_specs=[pl.BlockSpec(memory_space=pltpu.VMEM)] * len(outs),
        compiler_params=pltpu.CompilerParams(vmem_limit_bytes=12 * 2**20),
        cost_estimate=pl.CostEstimate(flops=600_000_000, bytes_accessed=0, transcendentals=0),
    )(*([] if where is None else [where]), *inputs)


def shards(acts_in, grad_query, attn_out, grad_out, row_query, col_query, row_output, col_output):
    query_rows = row_query.shape[0]
    output_rows = row_output.shape[0]
    query_width = col_query.shape[0]
    output_width = col_output.shape[0]
    y, z, core = lax.axis_index(Y), lax.axis_index(Z), lax.axis_index(CORE)
    pair_query, pair_output = 2 * query_rows, 2 * output_rows
    where = jnp.stack(
        [core]
        + [lax.rem(y + k, 4) * (4 * pair_query) for k in range(4)]
        + [lax.rem(z + k, 4) * pair_output for k in range(4)]
        + [lax.rem(k + 4 - z, 4) for k in range(4)]
        + [lax.rem(y + k, 4) for k in range(4)]
    ).astype(jnp.int32)

    def made(kernel, where, left, right, ks, group, vmem):
        kept, give = partial_blocks(kernel, where, left, right, ks, group, vmem)
        return kept, flat(kept), flat(shift(give, CORE, 1))

    def query_blocks(where, ks, vmem):
        return made(query_kernel, where, acts_in, grad_query, ks, query_rows, vmem)

    def output_blocks(where, ks, vmem):
        return made(output_kernel, where, attn_out, grad_out, ks, output_rows, vmem)

    one, two = (2, 1), (3, 0)
    far_plan = [[[(0, e), (1, e)] for e in half] for half in (one, two)]

    def near_plan(half, relayed):
        plan = [[[(0, base + e), (1, base + e)] for e in half] for base in (0, 4)]
        for i, terms in enumerate(plan[relayed]):
            terms.append((2, i))
        return plan

    last_one = [[[(0, e), (1, e), (2, i), (3, i)]] for i, e in enumerate(one)]
    last_two = [[[(0, e), (1, e), (2, i), (3, i)]] for i, e in enumerate(two)]

    query_made, *query_block = query_blocks(where, (2,), GRANTS[0])
    output_made, *output_block = output_blocks(after(where, query_made), (2,), GRANTS[1])
    query_far_one, query_far_two = add_entries(query_block, far_plan)
    query_low = shift(query_far_one, Y, 1)
    query_high = shift(query_far_two, Y, -1)
    output_far_one, output_far_two = add_entries(output_block, far_plan)
    output_low = shift(output_far_one, Z, 1)
    output_high = shift(output_far_two, Z, -1)

    ready = after(where, query_far_one, output_far_one)
    query_made, *query_block = query_blocks(ready, (1, 3), GRANTS[2])
    output_made, *output_block = output_blocks(after(where, query_made), (1, 3), GRANTS[3])

    def near(block, arrived, half, relayed, axis):
        plus, minus = add_entries((*block, arrived), near_plan(half, relayed))
        return plus, (shift(plus, axis, 1), shift(minus, axis, -1))

    query_plus, query_one = near(query_block, query_low, one, 0, Y)
    output_plus, output_one = near(output_block, output_low, one, 0, Z)
    query_plus, query_two = near(query_block, query_high, two, 1, Y)
    output_plus, output_two = near(output_block, output_high, two, 1, Z)

    ready = after(where, query_plus, output_plus)
    output_made, *output_block = output_blocks(ready, (0,), GRANTS[4])
    query_made, *query_block = query_blocks(after(where, output_made), (0,), GRANTS[5])
    wide_own = [jnp.bfloat16, jnp.float32]
    query_2, query_1 = add_entries((*query_block, *query_one), last_one)
    query_sent = [shift(query_2, Z, 2), shift(query_1, Z, 1)]
    output_2, output_1 = add_entries((*output_block, *output_one), last_one)
    output_sent = [shift(output_2, Y, 2), shift(output_1, Y, 1)]
    query_3, query_own = add_entries((*query_block, *query_two), last_two, wide_own)
    query_sent.append(shift(query_3, Z, 3))
    output_3, output_own = add_entries((*output_block, *output_two), last_two, wide_own)
    output_sent.append(shift(output_3, Y, 3))
    query_grad = query_own[0] + sum(wide(p[0]) for p in query_sent)
    output_grad = output_own[0] + sum(wide(p[0]) for p in output_sent)

    query_rowsum, query_colsum = sums_of(query_grad)
    output_rowsum, output_colsum = sums_of(output_grad)
    line = lambda value: value.reshape(1, -1)
    split = -(-query_rows // 128) * 128
    rows = line(
        jnp.concatenate(
            [query_rowsum, jnp.zeros((split - query_rows,), jnp.float32), output_rowsum]
        )
    )
    width = -(-(query_width + output_width) // 256) * 128
    packet = ((1, width + 128), jnp.float32)
    sums = [line(v) for v in (query_colsum, output_colsum, row_query, row_output)]
    keep, give = small_call(
        functools.partial(halves_kernel, split), [packet, packet], rows, *sums, where=where
    )
    got = shift(give, CORE, 1)
    half = keep + got
    for axis in (Y, Z):
        half = four(half, *exchanged(half, axis))
    other = shift(half[:, :width], CORE, 1)
    rows = jnp.concatenate([rows, half[:, width:]], axis=1)
    others = exchanged(rows, X)
    olds = [line(v) for v in (row_query, col_query, row_output, col_output)]
    update_query, new_row_query, new_col_query, update_output, new_row_output, new_col_output = small_call(
        functools.partial(finish_kernel, split, lax.axis_size(X), lax.axis_size(ROW)),
        [
            (query_grad.shape, jnp.bfloat16),
            (olds[0].shape, jnp.float32),
            (olds[1].shape, jnp.float32),
            (output_grad.shape, jnp.bfloat16),
            (olds[2].shape, jnp.float32),
            (olds[3].shape, jnp.float32),
        ],
        half,
        other,
        rows,
        *others,
        *olds,
        query_grad,
        output_grad,
        where=where,
    )
    return (
        update_query,
        update_output,
        new_row_query.reshape(-1),
        new_col_query.reshape(-1),
        new_row_output.reshape(-1),
        new_col_output.reshape(-1),
    )


def solution(mesh):
    split = Mesh(
        mesh.devices.reshape(4, 4, 2, mesh.shape[X]), (Y, Z, CORE, X)
    )
    return jax.shard_map(
        shards,
        mesh=split,
        in_specs=(
            P(ROW, None),
            P(ROW, X),
            P(ROW, None),
            P(ROW, X),
            P(ROW),
            P(X),
            P(ROW),
            P(X),
        ),
        out_specs=(P(ROW, X), P(ROW, X), P(ROW), P(X), P(ROW), P(X)),
        check_vma=False,
    )
```

```python
import functools

import jax
import jax.numpy as jnp
from jax import lax
from jax.experimental import pallas as pl
from jax.experimental.pallas import tpu as pltpu
from jax.sharding import Mesh
from jax.sharding import PartitionSpec as P


CLIP = 3072
Y, Z, CORE, X = "row_0", "row_1", "row_2", "col"
ROW = (Y, Z, CORE)

GRANTS = 30, 30, 12, 12, 12, 12
decay_rate = 0.81
epsilon_one = 1e-30


def shift(value, axis, by):
    size = lax.axis_size(axis)
    return lax.ppermute(value, axis, [(i, (i + by) % size) for i in range(size)])


def dot_rows(left, right_ref):
    product = lax.dot_general(
        left, right_ref[...], (((0,), (0,)), ((), ())), preferred_element_type=jnp.float32
    )
    return product.astype(jnp.bfloat16)


def query_kernel(first, group, where_ref, left_ref, right_ref, keep_ref, give_ref):
    core = where_ref[0]
    width = 8 * group // 3

    def block(b, carry):
        start = where_ref[1 + first + 2 * b]
        for side in (0, 1):

            @pl.when(core == side)
            def _(side=side):
                for s in range(3):
                    columns = pl.ds(pl.multiple_of(start + s * width, 128), width)
                    product = dot_rows(left_ref[:, columns], right_ref)
                    for j in range(8):
                        low, high = max(j * group, s * width), min((j + 1) * group, (s + 1) * width)
                        if low < high:
                            target = keep_ref if j % 2 == side else give_ref
                            rows = slice(low - j * group, high - j * group)
                            piece = product[low - s * width : high - s * width]
                            target[b, where_ref[9 + j // 2], rows, :] = piece

        return carry

    lax.fori_loop(0, keep_ref.shape[0], block, 0)


def output_kernel(first, group, where_ref, left_ref, right_ref, keep_ref, give_ref):
    core = where_ref[0]

    def block(b, carry):
        start = where_ref[5 + first + 2 * b]
        for half, target in ((1 - core, give_ref), (core, keep_ref)):
            runs = [
                left_ref[
                    :,
                    pl.ds(
                        pl.multiple_of(
                            start + where_ref[13 + e] * (8 * group) + half * group, 128
                        ),
                        group,
                    ),
                ]
                for e in range(4)
            ]
            product = dot_rows(jnp.concatenate(runs, axis=1), right_ref)
            for e in range(4):
                target[b, e] = product[e * group : (e + 1) * group]
        return carry

    lax.fori_loop(0, keep_ref.shape[0], block, 0)


def partial_blocks(kernel, where, left, right, blocks, group, vmem):
    tokens, columns = right.shape
    shape = jax.ShapeDtypeStruct((len(blocks), 4, group, columns), jnp.bfloat16)
    rows = 8 * group * len(blocks)
    return pl.pallas_call(
        functools.partial(kernel, blocks[0], group),
        out_shape=[shape, shape],
        in_specs=[pl.BlockSpec(memory_space=pltpu.SMEM)]
        + [pl.BlockSpec(memory_space=pltpu.VMEM)] * 2,
        out_specs=[pl.BlockSpec(memory_space=pltpu.VMEM)] * 2,
        compiler_params=pltpu.CompilerParams(vmem_limit_bytes=vmem * 2**20),
        cost_estimate=pl.CostEstimate(
            flops=2 * rows * tokens * columns, bytes_accessed=2 * rows * tokens, transcendentals=0
        ),
    )(where, left, right)


def add_kernel(plan, step, *refs):
    inputs, outputs = refs[: len(refs) - len(plan)], refs[len(refs) - len(plan) :]
    rows = outputs[0].shape[1]
    for o, entries in enumerate(plan):
        for e, terms in enumerate(entries):

            def chunk(i, carry, o=o, e=e, terms=terms):
                at = pl.ds(pl.multiple_of(i * step, step), step)
                value = None
                for which, entry in terms:
                    term = inputs[which][entry, at, :].astype(jnp.float32)
                    value = term if value is None else value + term
                outputs[o][e, at, :] = value.astype(outputs[o].dtype)
                return carry

            lax.fori_loop(0, rows // step, chunk, 0)


def add_entries(inputs, plan, dtypes=None):
    rows, columns = inputs[0].shape[1:]
    dtypes = dtypes or [jnp.bfloat16] * len(plan)
    return pl.pallas_call(
        functools.partial(add_kernel, plan, 16),
        out_shape=[jax.ShapeDtypeStruct((len(p), rows, columns), d) for p, d in zip(plan, dtypes)],
        in_specs=[pl.BlockSpec(memory_space=pltpu.VMEM)] * len(inputs),
        out_specs=[pl.BlockSpec(memory_space=pltpu.VMEM)] * len(plan),
        cost_estimate=pl.CostEstimate(flops=600_000_000, bytes_accessed=0, transcendentals=0),
        compiler_params=pltpu.CompilerParams(vmem_limit_bytes=12 * 2**20),
    )(*inputs)


def wide(value):
    return value.astype(jnp.float32)


def after(value, *others):
    return lax.optimization_barrier((value, *others))[0]


def flat(value):
    return value.reshape(-1, *value.shape[2:])


def sums_of(gradient):
    square = gradient * gradient
    return jnp.sum(square, axis=1), jnp.sum(square, axis=0)


def pack_kernel(split, *refs):
    rows_refs, (query_cols, output_cols, query_old, output_old, rows_ref, packed_ref) = refs[:4], refs[4:]
    total = rows_refs[0][...] + rows_refs[1][...] + rows_refs[2][...] + rows_refs[3][...]
    rows_ref[...] = total
    lane = lax.broadcasted_iota(jnp.int32, (1, 128), 1)
    scalars = jnp.zeros((1, 128), jnp.float32)
    parts = (total[:, :split], total[:, split:], query_old[...], output_old[...])
    for i, part in enumerate(parts):
        scalars = jnp.where(lane == i, jnp.sum(part, axis=1, keepdims=True), scalars)
    row = jnp.concatenate([query_cols[...], output_cols[...], scalars], axis=1)
    for i in range(packed_ref.shape[0]):
        packed_ref[i] = row


def finish_kernel(
    split,
    across,
    along,
    sums_ref,
    rows_ref,
    query_row,
    query_col,
    output_row,
    output_col,
    query_grad,
    output_grad,
    query_update,
    query_row_new,
    query_col_new,
    output_update,
    output_row_new,
    output_col_new,
):
    sums = sums_ref[0]
    for i in range(1, sums_ref.shape[0]):
        sums = sums + sums_ref[i]
    query_width, output_width = query_col.shape[1], output_col.shape[1]
    lane = lax.broadcasted_iota(jnp.int32, (1, 128), 1)
    tail = sums[:, query_width + output_width :]
    query_squares, output_squares, query_old, output_old = (
        jnp.sum(jnp.where(lane == i, tail, 0.0), axis=1, keepdims=True) for i in range(4)
    )
    norm = jnp.sqrt(query_squares + output_squares)
    clip_scale = CLIP / jnp.maximum(norm, jnp.float32(CLIP))
    squared_scale = clip_scale * clip_scale

    def one(at, offset, squares, old, row, col, grad, update, row_new, col_new):
        rows, columns = grad.shape
        whole_rows, whole_cols = rows * along, columns * across
        fresh = 1.0 - decay_rate

        def mean(value, count):
            return squared_scale * value / count + epsilon_one

        level = decay_rate * old / whole_rows + fresh * mean(squares, whole_rows * whole_cols)
        row_next = decay_rate * row[...] + fresh * mean(rows_ref[:, at : at + rows], whole_cols)
        col_next = decay_rate * col[...] + fresh * mean(sums[:, offset : offset + columns], whole_rows)
        row_new[...] = row_next
        col_new[...] = col_next
        square = (rows, rows)
        diagonal = lax.broadcasted_iota(jnp.int32, square, 0) == lax.broadcasted_iota(
            jnp.int32, square, 1
        )
        down = jnp.sum(jnp.where(diagonal, row_next, 0.0), axis=1, keepdims=True)
        scale = clip_scale * lax.rsqrt(down / level)
        update[...] = (grad[...] * scale * lax.rsqrt(col_next)).astype(jnp.bfloat16)

    one(
        0, 0, query_squares, query_old,
        query_row, query_col, query_grad, query_update, query_row_new, query_col_new,
    )
    one(
        split, query_width, output_squares, output_old,
        output_row, output_col, output_grad, output_update, output_row_new, output_col_new,
    )


def small_call(kernel, outs, *inputs):
    return pl.pallas_call(
        kernel,
        out_shape=[jax.ShapeDtypeStruct(shape, dtype) for shape, dtype in outs],
        in_specs=[pl.BlockSpec(memory_space=pltpu.VMEM)] * len(inputs),
        out_specs=[pl.BlockSpec(memory_space=pltpu.VMEM)] * len(outs),
        compiler_params=pltpu.CompilerParams(vmem_limit_bytes=12 * 2**20),
        cost_estimate=pl.CostEstimate(flops=600_000_000, bytes_accessed=0, transcendentals=0),
    )(*inputs)


def shards(acts_in, grad_query, attn_out, grad_out, row_query, col_query, row_output, col_output):
    query_rows = row_query.shape[0]
    output_rows = row_output.shape[0]
    query_width = col_query.shape[0]
    output_width = col_output.shape[0]
    y, z, core = lax.axis_index(Y), lax.axis_index(Z), lax.axis_index(CORE)
    pair_query, pair_output = 2 * query_rows, 2 * output_rows
    where = jnp.stack(
        [core]
        + [lax.rem(y + k, 4) * (4 * pair_query) for k in range(4)]
        + [lax.rem(z + k, 4) * pair_output for k in range(4)]
        + [lax.rem(k + 4 - z, 4) for k in range(4)]
        + [lax.rem(y + k, 4) for k in range(4)]
    ).astype(jnp.int32)

    def made(kernel, where, left, right, ks, group, vmem):
        kept, give = partial_blocks(kernel, where, left, right, ks, group, vmem)
        return kept, flat(kept), flat(shift(give, CORE, 1))

    def query_blocks(where, ks, vmem):
        return made(query_kernel, where, acts_in, grad_query, ks, query_rows, vmem)

    def output_blocks(where, ks, vmem):
        return made(output_kernel, where, attn_out, grad_out, ks, output_rows, vmem)

    one, two = (2, 1), (3, 0)
    far_plan = [[[(0, e), (1, e)] for e in half] for half in (one, two)]

    forward, stay = (2, 1, 3), (0,)

    def near_plan(entries):
        plus, minus = [], []
        for e in entries:
            own_plus, own_minus = [(0, e), (1, e)], [(0, 4 + e), (1, 4 + e)]
            plus.append(own_plus + ([(2, one.index(e))] if e in one else []))
            minus.append(own_minus + ([(3, two.index(e))] if e in two else []))
        return [plus, minus]

    last_one, last_two = (
        [[[(0, e), (1, e), (2, i), (3, i)]] for i, e in enumerate(half)] for half in (forward, stay)
    )

    query_made, *query_block = query_blocks(where, (2,), GRANTS[0])
    output_made, *output_block = output_blocks(after(where, query_made), (2,), GRANTS[1])
    query_far_one, query_far_two = add_entries(query_block, far_plan)
    query_low = shift(query_far_one, Y, 1)
    query_high = shift(query_far_two, Y, -1)
    output_far_one, output_far_two = add_entries(output_block, far_plan)
    output_low = shift(output_far_one, Z, 1)
    output_high = shift(output_far_two, Z, -1)

    ready = after(where, query_far_one, output_far_one)
    query_made, *query_block = query_blocks(ready, (1, 3), GRANTS[2])
    output_made, *output_block = output_blocks(after(where, query_made), (1, 3), GRANTS[3])

    def near(block, arrived, entries, axis):
        plus, minus = add_entries((*block, *arrived), near_plan(entries))
        return plus, (shift(plus, axis, 1), shift(minus, axis, -1))

    query_far, output_far = (query_low, query_high), (output_low, output_high)
    query_plus, query_one = near(query_block, query_far, forward, Y)
    output_plus, output_one = near(output_block, output_far, forward, Z)
    query_plus, query_two = near(query_block, query_far, stay, Y)
    output_plus, output_two = near(output_block, output_far, stay, Z)

    ready = after(where, query_plus, output_plus)
    query_made, *query_block = query_blocks(ready, (0,), GRANTS[4])
    output_made, *output_block = output_blocks(after(where, query_made), (0,), GRANTS[5])
    sends = add_entries((*output_block, *output_one), last_one)
    output_sent = [shift(v, Y, k) for k, v in zip(forward, sends)]
    sends = add_entries((*query_block, *query_one), last_one)
    query_sent = [shift(v, Z, k) for k, v in zip(forward, sends)]
    (query_own,) = add_entries((*query_block, *query_two), last_two, [jnp.float32])
    (output_own,) = add_entries((*output_block, *output_two), last_two, [jnp.float32])
    query_grad = query_own[0] + sum(wide(p[0]) for p in query_sent)
    output_grad = output_own[0] + sum(wide(p[0]) for p in output_sent)

    query_rowsum, query_colsum = sums_of(query_grad)
    output_rowsum, output_colsum = sums_of(output_grad)
    line = lambda value: value.reshape(1, -1)
    split = -(-query_rows // 128) * 128
    rows = line(
        jnp.concatenate(
            [query_rowsum, jnp.zeros((split - query_rows,), jnp.float32), output_rowsum]
        )
    )
    others = [shift(rows, X, k) for k in (2, 1, 3)]
    width = query_width + output_width + 128
    rows, packed = small_call(
        functools.partial(pack_kernel, split),
        [(rows.shape, jnp.float32), ((lax.axis_size(ROW), 1, width), jnp.float32)],
        rows,
        *others,
        *(line(v) for v in (query_colsum, output_colsum, row_query, row_output)),
    )
    packed = lax.all_to_all(packed, ROW, 0, 0, tiled=True)
    olds = [line(v) for v in (row_query, col_query, row_output, col_output)]
    update_query, new_row_query, new_col_query, update_output, new_row_output, new_col_output = small_call(
        functools.partial(finish_kernel, split, lax.axis_size(X), lax.axis_size(ROW)),
        [
            (query_grad.shape, jnp.bfloat16),
            (olds[0].shape, jnp.float32),
            (olds[1].shape, jnp.float32),
            (output_grad.shape, jnp.bfloat16),
            (olds[2].shape, jnp.float32),
            (olds[3].shape, jnp.float32),
        ],
        packed,
        rows,
        *olds,
        query_grad,
        output_grad,
    )
    return (
        update_query,
        update_output,
        new_row_query.reshape(-1),
        new_col_query.reshape(-1),
        new_row_output.reshape(-1),
        new_col_output.reshape(-1),
    )


def solution(mesh):
    split = Mesh(
        mesh.devices.reshape(4, 4, 2, mesh.shape[X]), (Y, Z, CORE, X)
    )
    return jax.shard_map(
        shards,
        mesh=split,
        in_specs=(
            P(ROW, None),
            P(ROW, X),
            P(ROW, None),
            P(ROW, X),
            P(ROW),
            P(X),
            P(ROW),
            P(X),
        ),
        out_specs=(P(ROW, X), P(ROW, X), P(ROW), P(X), P(ROW), P(X)),
        check_vma=False,
    )
```
